256 devices in a mesh: slides: 2 (over y), row: 128 (over x, z, core).
Axes of the slice: x: 4, y: 2, z: 16, core: 2. Of those that a mesh axis runs over, the one named last changes fastest.
The devices are a block of a 4x16x16 slice.
Arguments:
- slide_pixels: bfloat16 [16384, 16384], P(('slides', 'row')), parts along dimension 0, may hold values from -6 to 6
- tissue_mask: int32 [512, 8], P(('slides', 'row')), parts along dimension 0, may hold values from 0 to 1, as said below
- conv_weight: bfloat16 [3, 3, 64, 64], replicated, may hold values from -0.25 to 0.25
- conv_bias: bfloat16 [64], replicated, may hold values from -3 to 3
Outputs:
- packed_tiles: bfloat16 [2048, 32, 2048], P(('slides', 'row')), parts along dimension 0
The draws below stay inside these ranges and needn't reach their ends.
There are 2 independent parts, one for each index of `slides`. The reference program is written for one: setup_inputs(seed, part) draws one part's arguments, and reference() takes and returns one part's arrays. A program takes and returns all parts, laid end to end along the dimension named above; an argument that names none is the same for every part. Nothing has to cross between parts.
Inputs may be any that keep to these rules, and one draw needn't show every extreme that they name: `tissue_mask`: exactly 1024 tiles hold tissue. For every s from 1 to 127, the first s * 2 tile rows hold s * 8 + e tissue tiles with e between 0 and 2; e = 2 occurs in every draw. For every such s, some column holds tissue in both tile row s * 2 - 1 and tile row s * 2.
All inputs are finite; a program needn't handle non-finite values.
Results may differ from the reference program's by a relative error of at most 0.001.
Values may be sent and summed in bfloat16 or wider, within the bound.
A program may use at most 64 MiB of HBM per device.

```python
import jax
import jax.numpy as jnp
from jax import lax

CH = 64
SIDE = 32
SLOTS = 8
ROWS_DEV = 2
COLS = 8
SHIFT_MOST = 2
GRID_ROWS = 256
N_ROW = 128


def draw_tissue_mask(key, part):
    walk_key, first_key, order_key, column_key = jax.random.split(jax.random.fold_in(key, 7), 4)
    device_total = N_ROW
    reach_most = SHIFT_MOST
    drift_walk = jax.random.randint(walk_key, (device_total + 1,), 0, reach_most + 1)
    first_step = jax.random.randint(first_key, (), 1, device_total)
    step_index = jnp.arange(device_total + 1)
    drift_walk = jnp.where(step_index == first_step, reach_most, drift_walk)
    middle = device_total // 2
    in_window = (step_index >= middle - 2) & (step_index <= middle + 3)
    alternating = step_index % 2 * reach_most
    drift_walk = jnp.where(in_window, alternating, drift_walk)
    drift_walk = jnp.where((step_index == 0) | (step_index == device_total), 0, drift_walk)
    counts = SLOTS + drift_walk[1:] - drift_walk[:-1]
    tiles_band = ROWS_DEV * COLS
    boundary_cols = jax.random.randint(column_key, (device_total + 1,), 0, COLS)
    tile_index = jnp.arange(tiles_band)
    top_forced = tile_index[None, :] == boundary_cols[:-1, None]
    bottom_forced = tile_index[None, :] == (ROWS_DEV - 1) * COLS + boundary_cols[1:, None]
    band_index = jnp.arange(device_total)[:, None]
    forced = top_forced & (band_index > 0) | bottom_forced & (band_index < device_total - 1)
    scores = jax.random.randint(order_key, (device_total, tiles_band), 0, 1 << 20) * tiles_band
    scores = scores + tile_index[None, :]
    scores = jnp.where(forced, -1 - tile_index[None, :], scores)
    ranking = jnp.argsort(jnp.argsort(scores, axis=1), axis=1)
    tissue = (ranking < counts[:, None]).astype(jnp.int32)
    return tissue.reshape(device_total * ROWS_DEV, COLS)


def steps_of(key, dims, cuts, smallest, largest):
    loudness, own = 1.0, jax.random.fold_in(key, 6)
    for dim, parts in cuts:
        steps = jnp.exp(jax.random.uniform(jax.random.fold_in(own, dim), (parts,), jnp.float32, smallest / len(cuts), largest / len(cuts)))
        loudness = loudness * jnp.repeat(steps, dims[dim] // parts).reshape([-1 if axis == dim else 1 for axis in range(len(dims))])
    return loudness


def noise(stream_key, extent, width, bound, cuts=(), held_as=jnp.bfloat16):
    loudness = steps_of(stream_key, extent, cuts, -0.22, 0.18) if cuts else 1.0
    array = jax.random.normal(stream_key, extent, jnp.float32) * width * loudness
    return jnp.minimum(jnp.maximum(array, -bound), bound).astype(held_as)


def setup_inputs(seed: int = 0, part: int = 0) -> dict:
    key_of = jax.random.split(jax.random.key(seed), 5)
    own_keys = jax.random.split(jax.random.fold_in(key_of[4], part), 5)
    slide_pixels = noise(own_keys[0], (GRID_ROWS * SIDE, COLS * SIDE * CH), 1.0, 6.0, ((0, 128),))
    tissue_mask = draw_tissue_mask(jax.random.fold_in(jax.random.fold_in(key_of[4], part), 71), part)
    conv_weight = noise(key_of[2], (3, 3, CH, CH), (9 * CH) ** -0.5, 0.25)
    conv_bias = noise(key_of[3], (CH,), 0.5, 3.0)
    return dict(slide_pixels=slide_pixels, tissue_mask=tissue_mask, conv_weight=conv_weight, conv_bias=conv_bias)


def reference(slide_pixels, tissue_mask, conv_weight, conv_bias):
    grid_rows, grid_cols = tissue_mask.shape
    channels = conv_weight.shape[2]
    side = slide_pixels.shape[0] // grid_rows
    image = slide_pixels.reshape(grid_rows * side, grid_cols * side, channels)
    flat_mask = tissue_mask.reshape(grid_rows * grid_cols)
    order = jnp.argsort(1 - flat_mask, stable=True)[: N_ROW * SLOTS].astype(jnp.int32)
    weight_full = conv_weight.astype(jnp.float32)
    bias_full = conv_bias.astype(jnp.float32)

    def one_tile(position):
        tile_row = position // grid_cols
        tile_col = position % grid_cols
        offsets = jnp.arange(side + 2, dtype=jnp.int32) - 1
        pixel_rows = tile_row * side + offsets
        pixel_cols = tile_col * side + offsets
        row_inside = (pixel_rows >= 0) & (pixel_rows < grid_rows * side)
        col_inside = (pixel_cols >= 0) & (pixel_cols < grid_cols * side)
        rows_safe = jnp.clip(pixel_rows, 0, grid_rows * side - 1).astype(jnp.int32)
        cols_safe = jnp.clip(pixel_cols, 0, grid_cols * side - 1).astype(jnp.int32)
        window = jnp.take(jnp.take(image, rows_safe, axis=0), cols_safe, axis=1).astype(jnp.float32)
        tissue = jnp.take(jnp.take(tissue_mask, rows_safe // side, axis=0), cols_safe // side, axis=1)
        living = row_inside[:, None] & col_inside[None, :] & (tissue == 1)
        window = jnp.where(living[:, :, None], window, jnp.zeros_like(window))
        result = jnp.zeros((side, side, channels), jnp.float32)
        for vertical in range(3):
            for horizontal in range(3):
                result = result + jnp.einsum(
                    "hwc,co->hwo",
                    window[vertical:vertical + side, horizontal:horizontal + side],
                    weight_full[vertical, horizontal],
                    precision=lax.Precision.HIGHEST)
        result = result + bias_full
        return result.astype(jnp.bfloat16).reshape(side, side * channels)

    return lax.map(one_tile, order)
```

```python
import functools

import jax
import jax.numpy as jnp
from jax import lax
from jax.experimental import pallas as pl
from jax.experimental.pallas import tpu as pltpu
from jax.sharding import Mesh
from jax.sharding import PartitionSpec as P

SLOTS = 8
SHIFT_MOST = 2
ROW = ("row_0", "row_1", "row_2")
SLIDES_ROW = ("slides", "row_0", "row_1", "row_2")
MESH = pl.DeviceIdType.MESH
LANES = 128
F32 = jnp.float32
BF16 = jnp.bfloat16
I32 = jnp.int32


def kernel(
    pixels,
    mask_in,
    weight_in,
    bias_in,
    out,
    band,
    mask,
    weight,
    bias,
    big,
    fat,
    lhs,
    done,
    edge_first,
    edge_last,
    first_row,
    last_row,
    first_send,
    last_send,
    above_in,
    below_in,
    above,
    below,
    tile_send,
    tile_in,
    rim_work,
    rim_send,
    rim_in,
    note_send,
    note_in,
    counts,
    line_send,
    line_in,
    order,
    local_sem,
    send_sem,
    recv_sem,
    many_sem,
):
    x, z, c = (lax.axis_index(axis) for axis in ROW)
    planes, ring, cores = (lax.axis_size(axis) for axis in ROW)
    rows_dev, cols = mask_in.shape
    side = pixels.shape[0] // rows_dev
    tiles = rows_dev * cols
    chunks = pixels.shape[1] // (cols * LANES)
    groups = chunks // 2
    total = cols * chunks
    rank = (x * ring + z) * cores + c
    group_size = planes * ring * cores
    early = z == 0
    hub = (z == 0) & (c == 1)
    pair = x + 1 - 2 * (x % 2)

    def place(r):
        r = (r + group_size) % group_size
        return {"row_0": r // (ring * cores), "row_1": (r // cores) % ring, "row_2": r % cores}

    nxt, prv = place(rank + 1), place(rank - 1)

    def tell(where):
        pl.semaphore_signal(barrier, inc=1, device_id=where, device_id_type=MESH)

    barrier = pltpu.get_barrier_semaphore()
    copies = [
        pltpu.make_async_copy(mask_in, mask, local_sem.at[0]),
        pltpu.make_async_copy(pixels.at[48:64], band.at[48:64], local_sem.at[1]),
        pltpu.make_async_copy(pixels.at[0:16], band.at[0:16], local_sem.at[2]),
        pltpu.make_async_copy(pixels.at[16:48], band.at[16:48], local_sem.at[3]),
        pltpu.make_async_copy(weight_in, weight, local_sem.at[4]),
        pltpu.make_async_copy(bias_in, bias, local_sem.at[5]),
    ]
    for copy in copies:
        copy.start()
    tell(nxt)
    tell(prv)

    @pl.when(hub)
    def _():
        tell({"row_0": pair, "row_1": z, "row_2": c})
        tell({"row_0": x, "row_1": z, "row_2": 0})
        tell({"row_0": pair, "row_1": z, "row_2": 0})

        def spread(k, _):
            for core in range(2):
                tell({"row_0": x, "row_1": k, "row_2": core})
                tell({"row_0": pair, "row_1": k, "row_2": core})
            return 0

        lax.fori_loop(1, ring, spread, 0)

    copies[0].wait()
    held = [mask[t // cols, t % cols] for t in range(tiles)]
    upto = []
    running = jnp.int32(0)
    for t in range(tiles):
        running = running + held[t]
        upto.append(running)
    own_count = running

    def nth(k):
        return sum(((upto[t] <= k).astype(I32) for t in range(tiles - 1)), jnp.int32(0))

    local = (x % 2) * (ring * cores) + z * cores + c
    counts[pl.ds(local, 1), :] = jnp.broadcast_to(own_count, (1, LANES))
    sent_tiles = [nth(own_count - SHIFT_MOST + a) for a in range(SHIFT_MOST)]
    for a in range(SHIFT_MOST):
        note_send[a : a + 1, :] = jnp.broadcast_to(sent_tiles[a], (1, LANES))
    for k in range(SLOTS):
        order[k] = nth(jnp.int32(k))

    def keep(row, col):
        inside = (col >= 0) & (col < cols)
        return jnp.where(inside, mask[row, jnp.clip(col, 0, cols - 1)], 0).astype(F32)

    lane = lax.broadcasted_iota(I32, (1, LANES), 1)
    lower = lane < LANES // 2

    copies[1].wait()
    copies[2].wait()
    zeros8 = jnp.zeros((8, LANES), F32)
    for ref in (first_row, last_row, above, below):
        ref[0:8, :] = zeros8
        ref[8 + total : 16 + total, :] = zeros8
    for col in range(cols):
        top_keep = held[col].astype(F32)
        low_keep = held[(rows_dev - 1) * cols + col].astype(F32)
        for k in range(chunks):
            at = col * chunks + k
            span = slice(at * LANES, (at + 1) * LANES)
            top = band[0:16, span].astype(F32)[0:1, :] * top_keep
            low = band[48:64, span].astype(F32)[15:16, :] * low_keep
            first_row[8 + at : 9 + at, :] = top
            last_row[8 + at : 9 + at, :] = low
    first_send[...] = first_row[8 : 8 + total, :].astype(BF16)
    last_send[...] = last_row[8 : 8 + total, :].astype(BF16)
    copies[3].wait()

    def lanes_of(col, k):
        at = jnp.clip(col * chunks + k, 0, total - 1)
        return pl.ds(at * LANES, LANES)

    for a in range(SHIFT_MOST):
        row, col = sent_tiles[a] // cols, sent_tiles[a] % cols
        rows = pl.ds(row * side, side)
        for k in range(chunks):
            tile_send[a, k] = band[rows, lanes_of(col, k)]
        right = band[rows, lanes_of(col, chunks)].astype(F32) * keep(row, col + 1)
        left = band[rows, lanes_of(col, -1)].astype(F32) * keep(row, col - 1)
        tile_send[a, chunks] = jnp.where(lower, right, left).astype(BF16)

    def one(source, pick):
        return source.astype(F32)[pick : pick + 1, :]

    def inner_rim(row, pick, block, col):
        centre = keep(row, col)
        for k in range(chunks):
            yield one(band[block : block + 16, lanes_of(col, k)], pick) * centre
        right = one(band[block : block + 16, lanes_of(col, chunks)], pick) * keep(row, col + 1)
        left = one(band[block : block + 16, lanes_of(col, -1)], pick) * keep(row, col - 1)
        yield jnp.where(lower, right, left)

    def edge_rim(ref, col):
        step = col * (chunks // 8) + 1
        body = ref[pl.ds(step * 8, chunks), :]
        for k in range(chunks):
            yield body[k : k + 1, :]
        left = ref[pl.ds((step - 1) * 8, 8), :][7:8, :]
        right = ref[pl.ds((step + chunks // 8) * 8, 8), :][0:1, :]
        yield jnp.where(lower, right, left)

    def build_big():
        copies[4].wait()
        copies[5].wait()
        nothing = jnp.zeros((64, 64), BF16)
        for dy in range(3):
            taps = [weight[dy, dx] for dx in range(3)]
            for p in (0, 1, 2, 3, 4, -1):
                parts = [taps[p - q + 1] if 0 <= p - q + 1 < 3 else nothing for q in range(4)]
                at = dy * 384 + (p if p >= 0 else 5) * 64
                big[at : at + 64, :] = jnp.concatenate(parts, axis=1)

    def bias_row():
        short = bias[...].astype(F32).reshape(1, 64)
        return jnp.concatenate([short] * 4, axis=1)

    def multiply():
        for dy in range(3):
            rows = slice(7 + dy, 7 + dy + side)
            for g in range(groups):
                at = slice(g * side, (g + 1) * side)
                right = fat[2 * g + 2 if g < groups - 1 else chunks, rows, :]
                left = fat[2 * g - 1 if g > 0 else chunks, rows, :]
                lhs[at, dy * 384 : dy * 384 + 128] = fat[2 * g, rows, :].astype(BF16)
                lhs[at, dy * 384 + 128 : dy * 384 + 256] = fat[2 * g + 1, rows, :].astype(BF16)
                lhs[at, dy * 384 + 256 : dy * 384 + 384] = jnp.where(lower, right, left).astype(BF16)
        return jnp.dot(lhs[...], big[...], preferred_element_type=F32) + bias_row()

    def finish(result, slot):
        for g in range(groups):
            done[slot, :, g * 256 : (g + 1) * 256] = result[g * side : (g + 1) * side].astype(BF16)

    def own_tiles():
        build_big()
        for row in range(rows_dev):

            def tile(col, _, row=row):
                rows = slice(row * side, (row + 1) * side)
                for k in range(chunks):
                    fat[k, 8 : 8 + side, :] = band[rows, lanes_of(col, k)].astype(F32)
                right = band[rows, lanes_of(col, chunks)].astype(F32) * keep(row, col + 1)
                left = band[rows, lanes_of(col, -1)].astype(F32) * keep(row, col - 1)
                fat[chunks, 8 : 8 + side, :] = jnp.where(lower, right, left)
                if row == 0:
                    rim = inner_rim(1, 0, side, col)
                    for k, line in enumerate(rim):
                        fat[k, 7:8, :] = jnp.zeros((1, LANES), F32)
                        fat[k, 8 + side : 9 + side, :] = line
                else:
                    rim = inner_rim(0, 15, side - 16, col)
                    for k, line in enumerate(rim):
                        fat[k, 7:8, :] = line
                        fat[k, 8 + side : 9 + side, :] = jnp.zeros((1, LANES), F32)
                result = multiply()
                finish(result, row * cols + col)
                for g in range(groups):
                    if row == 0:
                        edge_first[col, g : g + 1, :] = result[g * side : g * side + 1]
                    else:
                        edge_last[col, g : g + 1, :] = result[(g + 1) * side - 1 : (g + 1) * side]
                return 0

            lax.fori_loop(0, cols, tile, 0)

    @pl.when(early)
    def _():
        own_tiles()

    @pl.when(jnp.logical_not(hub))
    def _():
        pl.semaphore_wait(barrier, 4)

    @pl.when(hub)
    def _():
        pl.semaphore_wait(barrier, 3)

    def remote(source, target, k, where):
        return pltpu.make_async_remote_copy(
            source, target, send_sem.at[k], recv_sem.at[k], device_id=where, device_id_type=MESH
        )

    mine = counts.at[pl.ds(local, 1)]

    def count_to(plane):
        return pltpu.make_async_remote_copy(
            mine, mine, many_sem.at[0], many_sem.at[1],
            device_id={"row_0": plane, "row_1": 0, "row_2": 1}, device_id_type=MESH,
        )

    count_to(pair).start()

    @pl.when(jnp.logical_not(hub))
    def _():
        count_to(x).start()

    note = remote(note_send, note_in, 0, nxt)
    down = remote(last_send, above_in, 1, nxt)
    up = remote(first_send, below_in, 2, prv)
    bodies = [remote(tile_send.at[a], tile_in.at[a], 3 + a, nxt) for a in range(SHIFT_MOST)]
    rims = remote(rim_send, rim_in, 5, nxt)
    note.start()
    down.start()
    for body in bodies:
        body.start()
    up.start()

    def send_rims():
        down.wait_recv()
        seen = jnp.where(rank > 0, 1, 0).astype(F32)
        above[8 : 8 + total, :] = above_in[...].astype(F32) * seen
        row, col = sent_tiles[0] // cols, sent_tiles[0] % cols
        high = row == 0
        for k, (outer, inner) in enumerate(zip(edge_rim(above, col), inner_rim(0, 15, side - 16, col))):
            rim_work[0, k : k + 1, :] = jnp.where(high, outer, inner)
        for k, line in enumerate(inner_rim(1, 0, side, col)):
            rim_work[1, k : k + 1, :] = line
        for k, line in enumerate(inner_rim(0, 15, side - 16, sent_tiles[1] % cols)):
            rim_work[2, k : k + 1, :] = line
        rim_send[...] = rim_work[...].astype(BF16)
        rims.start()

    send_rims()

    @pl.when(jnp.logical_not(early))
    def _():
        own_tiles()

    up.wait_recv()
    seen = jnp.where(rank < group_size - 1, 1, 0).astype(F32)
    below[8 : 8 + total, :] = below_in[...].astype(F32) * seen

    def join(ref, edge, dy, row, block, pick):
        half = total // 2
        even = ref[pl.ds(8, half, 2), :]
        odd = ref[pl.ds(9, half, 2), :]
        right = ref[pl.ds(10, half, 2), :]
        left = ref[pl.ds(7, half, 2), :]
        side_by = jnp.concatenate([even, odd, jnp.where(lower, right, left)], axis=1).astype(BF16)
        more = jnp.dot(side_by, big[dy * 384 : (dy + 1) * 384, :], preferred_element_type=F32)
        at_row = lax.broadcasted_iota(I32, (16, 256), 0) == pick
        for col in range(cols):
            whole = more[col * groups : (col + 1) * groups] + edge[col]
            for g in range(groups):
                span = slice(g * 256, (g + 1) * 256)
                old = done[row * cols + col, block : block + 16, span].astype(F32)
                new = jnp.where(at_row, whole[g : g + 1, :], old)
                done[row * cols + col, block : block + 16, span] = new.astype(BF16)

    join(above, edge_first, 0, 0, 0, 0)
    join(below, edge_last, 2, rows_dev - 1, side - 16, 15)

    @pl.when(hub)
    def _():
        others = counts.at[pl.ds(0, 2 * ring * cores - 1)]
        pltpu.make_async_copy(others, others, many_sem.at[1]).wait()
        table = counts[...]
        spot = lax.broadcasted_iota(I32, table.shape, 0) == lax.broadcasted_iota(I32, table.shape, 1)
        line_send[...] = jnp.sum(jnp.where(spot, table, 0), axis=0, keepdims=True)

        def line_to(k, core):
            return pltpu.make_async_remote_copy(
                line_send, line_in, many_sem.at[2], many_sem.at[3],
                device_id={"row_0": x, "row_1": k, "row_2": core}, device_id_type=MESH,
            )

        line_to(0, 0).start()

        def spread(k, _):
            for core in range(2):
                line_to(k, core).start()
            return 0

        lax.fori_loop(1, ring, spread, 0)

    note.wait_recv()
    rims.wait_recv()
    for a in range(SHIFT_MOST):
        came = jnp.max(note_in[a : a + 1, :])
        row, col = came // cols, came % cols
        bodies[a].wait_recv()
        for k in range(chunks + 1):
            fat[k, 8 : 8 + side, :] = tile_in[a, k].astype(F32)
        over = rim_in[2 * a].astype(F32)
        under = rim_in[1].astype(F32)
        for k, line in enumerate(edge_rim(first_row, col)):
            fat[k, 7:8, :] = over[k : k + 1, :]
            if a == 0:
                line = jnp.where(row == rows_dev - 1, line, under[k : k + 1, :])
            fat[k, 8 + side : 9 + side, :] = line
        finish(multiply(), tiles + a)

    @pl.when(jnp.logical_not(hub))
    def _():
        pltpu.make_async_copy(line_in, line_in, many_sem.at[3]).wait()

    line = jnp.where(hub, line_send[...], line_in[...])
    before = jnp.sum(jnp.where(lane < local, line, 0))
    whole = jnp.sum(line)
    start = jnp.where(x < planes // 2, 0, SLOTS * ring * cores * 2 - whole)
    excess = start + before - SLOTS * local
    excess = jnp.clip(excess, 0, SHIFT_MOST)
    for j in range(SLOTS):
        own = order[jnp.clip(j - excess, 0, SLOTS - 1)]
        came = tiles + SHIFT_MOST - excess + j
        out[j] = done[jnp.clip(jnp.where(j < excess, came, own), 0, tiles + SHIFT_MOST - 1)]

    for copy in (note, down, up, *bodies, rims):
        copy.wait_send()
    count_to(pair).wait_send()

    @pl.when(jnp.logical_not(hub))
    def _():
        count_to(x).wait_send()

    @pl.when(hub)
    def _():
        sent = counts.at[pl.ds(0, ring * cores - 1)]
        pltpu.make_async_copy(sent, sent, many_sem.at[2]).wait()


def on_device(slide_pixels, tissue_mask, conv_weight, conv_bias):
    rows_dev, cols = tissue_mask.shape
    side = slide_pixels.shape[0] // rows_dev
    width = slide_pixels.shape[1] // cols
    chunks = width // LANES
    groups = chunks // 2
    total = cols * chunks
    tiles = rows_dev * cols
    pair_size = 2 * lax.axis_size("row_1") * lax.axis_size("row_2")
    strip = pltpu.VMEM((total + 16, LANES), F32)
    packed = pltpu.VMEM((total, LANES), BF16)
    rim = pltpu.VMEM((3, 32, LANES), BF16)
    tile_pair = pltpu.VMEM((SHIFT_MOST, chunks + 1, side, LANES), BF16)
    edge = pltpu.VMEM((cols, groups, 256), F32)
    return pl.pallas_call(
        kernel,
        out_shape=pltpu.VMEM((SLOTS, side, width), BF16),
        in_specs=[pl.BlockSpec(memory_space=pltpu.HBM)] * 4,
        out_specs=pl.BlockSpec(memory_space=pltpu.VMEM),
        scratch_shapes=[
            pltpu.VMEM(slide_pixels.shape, BF16),
            pltpu.SMEM((rows_dev, cols), I32),
            pltpu.VMEM(conv_weight.shape, BF16),
            pltpu.VMEM(conv_bias.shape, BF16),
            pltpu.VMEM((3 * 384, 256), BF16),
            pltpu.VMEM((chunks + 1, 48, LANES), F32),
            pltpu.VMEM((groups * side, 3 * 384), BF16),
            pltpu.VMEM((tiles + SHIFT_MOST, side, width), BF16),
            edge,
            edge,
            strip,
            strip,
            packed,
            packed,
            packed,
            packed,
            strip,
            strip,
            tile_pair,
            tile_pair,
            pltpu.VMEM((3, 32, LANES), F32),
            rim,
            rim,
            pltpu.VMEM((SHIFT_MOST, LANES), I32),
            pltpu.VMEM((SHIFT_MOST, LANES), I32),
            pltpu.VMEM((pair_size, LANES), I32),
            pltpu.VMEM((1, LANES), I32),
            pltpu.VMEM((1, LANES), I32),
            pltpu.SMEM((SLOTS,), I32),
            pltpu.SemaphoreType.DMA((6,)),
            pltpu.SemaphoreType.DMA((6,)),
            pltpu.SemaphoreType.DMA((6,)),
            pltpu.SemaphoreType.DMA((4,)),
        ],
        compiler_params=pltpu.CompilerParams(
            collective_id=0, has_side_effects=True, vmem_limit_bytes=24 * 1024 * 1024
        ),
        name="tissue_tiles",
    )(slide_pixels, tissue_mask, conv_weight, conv_bias)


def solution(mesh):
    finer = Mesh(
        mesh.devices.reshape(mesh.shape["slides"], 4, 16, 2), ("slides", "row_0", "row_1", "row_2")
    )
    return jax.shard_map(
        on_device,
        mesh=finer,
        in_specs=(P(SLIDES_ROW, None), P(SLIDES_ROW, None), P(), P()),
        out_specs=P(SLIDES_ROW, None, None),
        check_vma=False,
    )
```

```python
import functools

import jax
import jax.numpy as jnp
from jax import lax
from jax.experimental import pallas as pl
from jax.experimental.pallas import tpu as pltpu
from jax.sharding import Mesh
from jax.sharding import PartitionSpec as P

SLOTS = 8
SHIFT_MOST = 2
ROW = ("row_0", "row_1", "row_2")
SLIDES_ROW = ("slides", "row_0", "row_1", "row_2")
MESH = pl.DeviceIdType.MESH
LANES = 128
F32 = jnp.float32
BF16 = jnp.bfloat16
I32 = jnp.int32


def kernel(
    pixels,
    mask_in,
    weight_in,
    bias_in,
    out,
    top_band,
    low_band,
    mask,
    weight,
    bias,
    big,
    fat,
    lhs,
    done,
    edge_first,
    edge_last,
    first_row,
    last_row,
    first_send,
    last_send,
    above_in,
    below_in,
    above,
    below,
    tile_send,
    tile_in,
    rim_work,
    rim_send,
    rim_in,
    note_send,
    note_in,
    counts,
    line_send,
    line_in,
    order,
    local_sem,
    send_sem,
    recv_sem,
    many_sem,
):
    x, z, c = (lax.axis_index(axis) for axis in ROW)
    planes, ring, cores = (lax.axis_size(axis) for axis in ROW)
    rows_dev, cols = mask_in.shape
    side = pixels.shape[0] // rows_dev
    tiles = rows_dev * cols
    chunks = pixels.shape[1] // (cols * LANES)
    groups = chunks // 2
    total = cols * chunks
    rank = (x * ring + z) * cores + c
    group_size = planes * ring * cores
    follows, leads = rank > 0, rank < group_size - 1
    early = (z == 0) & follows
    hub = (z == 0) & (c == 1)
    pair = x + 1 - 2 * (x % 2)

    def place(r):
        r = (r + group_size) % group_size
        return {"row_0": r // (ring * cores), "row_1": (r // cores) % ring, "row_2": r % cores}

    nxt, prv = place(rank + 1), place(rank - 1)

    def tell(where):
        pl.semaphore_signal(barrier, inc=1, device_id=where, device_id_type=MESH)

    barrier = pltpu.get_barrier_semaphore()
    bands = (top_band, low_band)
    copies = [
        pltpu.make_async_copy(mask_in, mask, local_sem.at[0]),
        pltpu.make_async_copy(pixels.at[side : 2 * side], low_band, local_sem.at[1]),
        pltpu.make_async_copy(pixels.at[0:side], top_band, local_sem.at[2]),
        pltpu.make_async_copy(weight_in, weight, local_sem.at[3]),
        pltpu.make_async_copy(bias_in, bias, local_sem.at[4]),
    ]
    for copy in copies:
        copy.start()

    @pl.when(leads)
    def _():
        tell(nxt)

    @pl.when(follows)
    def _():
        tell(prv)

    @pl.when(hub)
    def _():
        tell({"row_0": pair, "row_1": z, "row_2": c})
        tell({"row_0": x, "row_1": z, "row_2": 0})
        tell({"row_0": pair, "row_1": z, "row_2": 0})

        def spread(k, _):
            for core in range(2):
                tell({"row_0": x, "row_1": k, "row_2": core})
                tell({"row_0": pair, "row_1": k, "row_2": core})
            return 0

        lax.fori_loop(1, ring, spread, 0)

    copies[0].wait()
    held = [mask[t // cols, t % cols] for t in range(tiles)]
    upto = []
    running = jnp.int32(0)
    for t in range(tiles):
        running = running + held[t]
        upto.append(running)
    own_count = running

    def nth(k):
        return sum(((upto[t] <= k).astype(I32) for t in range(tiles - 1)), jnp.int32(0))

    local = (x % 2) * (ring * cores) + z * cores + c
    counts[pl.ds(local, 1), :] = jnp.broadcast_to(own_count, (1, LANES))
    sent_tiles = [nth(own_count - SHIFT_MOST + a) for a in range(SHIFT_MOST)]
    for a in range(SHIFT_MOST):
        note_send[a : a + 1, :] = jnp.broadcast_to(sent_tiles[a], (1, LANES))
    def keep(row, col):
        inside = (col >= 0) & (col < cols)
        return jnp.where(inside, mask[row, jnp.clip(col, 0, cols - 1)], 0).astype(F32)

    lane = lax.broadcasted_iota(I32, (1, LANES), 1)
    lower = lane < LANES // 2

    def lanes_of(col, k):
        at = jnp.clip(col * chunks + k, 0, total - 1)
        return pl.ds(at * LANES, LANES)

    def outer_row(ref, send, row, block, pick):
        for col in range(cols):
            centre = held[row * cols + col].astype(F32)
            for k in range(chunks):
                at = col * chunks + k
                line = bands[row][block : block + 16, at * LANES : (at + 1) * LANES].astype(F32)
                ref[8 + at : 9 + at, :] = line[pick : pick + 1, :] * centre
        send[...] = ref[8 : 8 + total, :].astype(BF16)

    def stage(a):
        row, col = sent_tiles[a] // cols, sent_tiles[a] % cols
        row = row if a == 0 else rows_dev - 1

        def pixels_of(k):
            low = low_band[:, lanes_of(col, k)]
            return low if a else jnp.where(row == 0, top_band[:, lanes_of(col, k)], low)

        for k in range(chunks):
            tile_send[a, k] = pixels_of(k)
        right = pixels_of(chunks).astype(F32) * keep(row, col + 1)
        left = pixels_of(-1).astype(F32) * keep(row, col - 1)
        tile_send[a, chunks] = jnp.where(lower, right, left).astype(BF16)

    def one(source, pick):
        return source.astype(F32)[pick : pick + 1, :]

    def inner_rim(row, pick, block, col):
        centre = keep(row, col)
        for k in range(chunks):
            yield one(bands[row][block : block + 16, lanes_of(col, k)], pick) * centre
        right = one(bands[row][block : block + 16, lanes_of(col, chunks)], pick) * keep(row, col + 1)
        left = one(bands[row][block : block + 16, lanes_of(col, -1)], pick) * keep(row, col - 1)
        yield jnp.where(lower, right, left)

    def edge_rim(ref, col):
        step = col * (chunks // 8) + 1
        body = ref[pl.ds(step * 8, chunks), :]
        for k in range(chunks):
            yield body[k : k + 1, :]
        left = ref[pl.ds((step - 1) * 8, 8), :][7:8, :]
        right = ref[pl.ds((step + chunks // 8) * 8, 8), :][0:1, :]
        yield jnp.where(lower, right, left)

    def build_big():
        copies[3].wait()
        copies[4].wait()
        nothing = jnp.zeros((64, 64), BF16)
        for dy in range(3):
            taps = [weight[dy, dx] for dx in range(3)]
            for p in (0, 1, 2, 3, 4, -1):
                parts = [taps[p - q + 1] if 0 <= p - q + 1 < 3 else nothing for q in range(4)]
                at = dy * 384 + (p if p >= 0 else 5) * 64
                big[at : at + 64, :] = jnp.concatenate(parts, axis=1)

    def bias_row():
        short = bias[...].astype(F32).reshape(1, 64)
        return jnp.concatenate([short] * 4, axis=1)

    def multiply():
        for dy in range(3):
            rows = slice(7 + dy, 7 + dy + side)
            for g in range(groups):
                at = slice(g * side, (g + 1) * side)
                right = fat[2 * g + 2 if g < groups - 1 else chunks, rows, :]
                left = fat[2 * g - 1 if g > 0 else chunks, rows, :]
                lhs[at, dy * 384 : dy * 384 + 128] = fat[2 * g, rows, :].astype(BF16)
                lhs[at, dy * 384 + 128 : dy * 384 + 256] = fat[2 * g + 1, rows, :].astype(BF16)
                lhs[at, dy * 384 + 256 : dy * 384 + 384] = jnp.where(lower, right, left).astype(BF16)
        return jnp.dot(lhs[...], big[...], preferred_element_type=F32) + bias_row()

    def finish(result, slot):
        for g in range(groups):
            done[slot, :, g * 256 : (g + 1) * 256] = result[g * side : (g + 1) * side].astype(BF16)

    def own_tiles():
        build_big()
        for row in range(rows_dev):

            def tile(col, _, row=row):
                band = bands[row]
                for k in range(chunks):
                    fat[k, 8 : 8 + side, :] = band[:, lanes_of(col, k)].astype(F32)
                right = band[:, lanes_of(col, chunks)].astype(F32) * keep(row, col + 1)
                left = band[:, lanes_of(col, -1)].astype(F32) * keep(row, col - 1)
                fat[chunks, 8 : 8 + side, :] = jnp.where(lower, right, left)
                if row == 0:
                    rim = inner_rim(1, 0, 0, col)
                    for k, line in enumerate(rim):
                        fat[k, 7:8, :] = jnp.zeros((1, LANES), F32)
                        fat[k, 8 + side : 9 + side, :] = line
                else:
                    rim = inner_rim(0, 15, side - 16, col)
                    for k, line in enumerate(rim):
                        fat[k, 7:8, :] = line
                        fat[k, 8 + side : 9 + side, :] = jnp.zeros((1, LANES), F32)
                result = multiply()
                finish(result, row * cols + col)
                for g in range(groups):
                    if row == 0:
                        edge_first[col, g : g + 1, :] = result[g * side : g * side + 1]
                    else:
                        edge_last[col, g : g + 1, :] = result[(g + 1) * side - 1 : (g + 1) * side]
                return 0

            lax.fori_loop(0, cols, tile, 0)

    def remote(source, target, k, where):
        return pltpu.make_async_remote_copy(
            source, target, send_sem.at[k], recv_sem.at[k], device_id=where, device_id_type=MESH
        )

    mine = counts.at[pl.ds(local, 1)]

    def count_to(plane):
        return pltpu.make_async_remote_copy(
            mine, mine, many_sem.at[0], many_sem.at[1],
            device_id={"row_0": plane, "row_1": 0, "row_2": 1}, device_id_type=MESH,
        )

    def arrive():
        pl.semaphore_wait(barrier, 2 - hub.astype(I32) + follows.astype(I32) + leads.astype(I32))
        count_to(pair).start()

        @pl.when(jnp.logical_not(hub))
        def _():
            count_to(x).start()

    note = remote(note_send, note_in, 0, nxt)
    down = remote(last_send, above_in, 1, nxt)
    up = remote(first_send, below_in, 2, prv)
    bodies = [remote(tile_send.at[a], tile_in.at[a], 3 + a, nxt) for a in range(SHIFT_MOST)]
    fixed_rims = remote(rim_send.at[0:2], rim_in.at[0:2], 5, nxt)
    last_rim = remote(rim_send.at[2], rim_in.at[2], 6, nxt)
    def send_low():
        @pl.when(leads)
        def _():
            note.start()
            bodies[1].start()
            down.start()

    def send_top():
        stage(0)
        inner_rims()

        @pl.when(leads)
        def _():
            fixed_rims.start()
            bodies[0].start()

        outer_row(first_row, first_send, 0, 0, 0)

        @pl.when(follows)
        def _():
            up.start()

    def inner_rims():
        for k, line in enumerate(inner_rim(1, 0, 0, sent_tiles[0] % cols)):
            rim_work[0, k : k + 1, :] = line
        for k, line in enumerate(inner_rim(0, 15, side - 16, sent_tiles[1] % cols)):
            rim_work[1, k : k + 1, :] = line
        rim_send[0:2] = rim_work[0:2].astype(BF16)

    def send_last_rim():
        @pl.when(follows)
        def _():
            down.wait_recv()
            above[8 : 8 + total, :] = above_in[...].astype(F32)

        @pl.when(jnp.logical_not(follows))
        def _():
            above[8 : 8 + total, :] = jnp.zeros((total, LANES), F32)

        row, col = sent_tiles[0] // cols, sent_tiles[0] % cols
        for k, (outer, inner) in enumerate(zip(edge_rim(above, col), inner_rim(0, 15, side - 16, col))):
            rim_work[2, k : k + 1, :] = jnp.where(row == 0, outer, inner)
        rim_send[2] = rim_work[2].astype(BF16)

        @pl.when(leads)
        def _():
            last_rim.start()

    zeros8 = jnp.zeros((8, LANES), F32)
    for ref in (first_row, last_row, above, below):
        ref[0:8, :] = zeros8
        ref[8 + total : 16 + total, :] = zeros8

    @pl.when(jnp.logical_not(early))
    def _():
        arrive()

    copies[1].wait()
    stage(1)
    outer_row(last_row, last_send, rows_dev - 1, side - 16, 15)

    @pl.when(early)
    def _():
        copies[2].wait()
        own_tiles()
        arrive()
        send_low()
        send_top()

    @pl.when(jnp.logical_not(early))
    def _():
        send_low()
        copies[2].wait()
        send_top()
        send_last_rim()
        own_tiles()

    for k in range(SLOTS):
        order[k] = nth(jnp.int32(k))

    @pl.when(leads)
    def _():
        up.wait_recv()
        below[8 : 8 + total, :] = below_in[...].astype(F32)

    @pl.when(jnp.logical_not(leads))
    def _():
        below[8 : 8 + total, :] = jnp.zeros((total, LANES), F32)

    def join(ref, edge, dy, row, block, pick):
        half = total // 2
        even = ref[pl.ds(8, half, 2), :]
        odd = ref[pl.ds(9, half, 2), :]
        right = ref[pl.ds(10, half, 2), :]
        left = ref[pl.ds(7, half, 2), :]
        side_by = jnp.concatenate([even, odd, jnp.where(lower, right, left)], axis=1).astype(BF16)
        more = jnp.dot(side_by, big[dy * 384 : (dy + 1) * 384, :], preferred_element_type=F32)
        at_row = lax.broadcasted_iota(I32, (16, 256), 0) == pick
        for col in range(cols):
            whole = more[col * groups : (col + 1) * groups] + edge[col]
            for g in range(groups):
                span = slice(g * 256, (g + 1) * 256)
                old = done[row * cols + col, block : block + 16, span].astype(F32)
                new = jnp.where(at_row, whole[g : g + 1, :], old)
                done[row * cols + col, block : block + 16, span] = new.astype(BF16)

    join(below, edge_last, 2, rows_dev - 1, side - 16, 15)

    @pl.when(early)
    def _():
        send_last_rim()

    join(above, edge_first, 0, 0, 0, 0)

    @pl.when(hub)
    def _():
        others = counts.at[pl.ds(0, 2 * ring * cores - 1)]
        pltpu.make_async_copy(others, others, many_sem.at[1]).wait()
        table = counts[...]
        spot = lax.broadcasted_iota(I32, table.shape, 0) == lax.broadcasted_iota(I32, table.shape, 1)
        line_send[...] = jnp.sum(jnp.where(spot, table, 0), axis=0, keepdims=True)

        def line_to(k, core):
            return pltpu.make_async_remote_copy(
                line_send, line_in, many_sem.at[2], many_sem.at[3],
                device_id={"row_0": x, "row_1": k, "row_2": core}, device_id_type=MESH,
            )

        line_to(0, 0).start()

        def spread(k, _):
            for core in range(2):
                line_to(k, core).start()
            return 0

        lax.fori_loop(1, ring, spread, 0)

    def taken(a):
        came = jnp.max(note_in[a : a + 1, :])
        row, col = came // cols, came % cols
        bodies[a].wait_recv()
        for k in range(chunks + 1):
            fat[k, 8 : 8 + side, :] = tile_in[a, k].astype(F32)
        over = rim_in[1 if a else 2].astype(F32)
        under = rim_in[0].astype(F32)
        for k, line in enumerate(edge_rim(first_row, col)):
            fat[k, 7:8, :] = over[k : k + 1, :]
            if a == 0:
                line = jnp.where(row == rows_dev - 1, line, under[k : k + 1, :])
            fat[k, 8 + side : 9 + side, :] = line
        finish(multiply(), tiles + a)

    @pl.when(follows)
    def _():
        note.wait_recv()
        fixed_rims.wait_recv()
        taken(1)
        last_rim.wait_recv()
        taken(0)

    @pl.when(jnp.logical_not(hub))
    def _():
        pltpu.make_async_copy(line_in, line_in, many_sem.at[3]).wait()

    line = jnp.where(hub, line_send[...], line_in[...])
    before = jnp.sum(jnp.where(lane < local, line, 0))
    whole = jnp.sum(line)
    start = jnp.where(x < planes // 2, 0, SLOTS * ring * cores * 2 - whole)
    excess = start + before - SLOTS * local
    excess = jnp.clip(excess, 0, SHIFT_MOST)
    for j in range(SLOTS):
        own = order[jnp.clip(j - excess, 0, SLOTS - 1)]
        came = tiles + SHIFT_MOST - excess + j
        out[j] = done[jnp.clip(jnp.where(j < excess, came, own), 0, tiles + SHIFT_MOST - 1)]

    @pl.when(leads)
    def _():
        for copy in (note, down, *bodies, fixed_rims, last_rim):
            copy.wait_send()

    @pl.when(follows)
    def _():
        up.wait_send()

    count_to(pair).wait_send()

    @pl.when(jnp.logical_not(hub))
    def _():
        count_to(x).wait_send()

    @pl.when(hub)
    def _():
        sent = counts.at[pl.ds(0, ring * cores - 1)]
        pltpu.make_async_copy(sent, sent, many_sem.at[2]).wait()


def in_hbm(array):
    return pltpu.with_memory_space_constraint(array, pltpu.HBM)


def on_device(slide_pixels, tissue_mask, conv_weight, conv_bias):
    rows_dev, cols = tissue_mask.shape
    side = slide_pixels.shape[0] // rows_dev
    width = slide_pixels.shape[1] // cols
    chunks = width // LANES
    groups = chunks // 2
    total = cols * chunks
    tiles = rows_dev * cols
    pair_size = 2 * lax.axis_size("row_1") * lax.axis_size("row_2")
    half = pltpu.VMEM((side, slide_pixels.shape[1]), BF16)
    strip = pltpu.VMEM((total + 16, LANES), F32)
    packed = pltpu.VMEM((total, LANES), BF16)
    rim = pltpu.VMEM((3, 32, LANES), BF16)
    tile_pair = pltpu.VMEM((SHIFT_MOST, chunks + 1, side, LANES), BF16)
    edge = pltpu.VMEM((cols, groups, 256), F32)
    return pl.pallas_call(
        kernel,
        out_shape=pltpu.VMEM((SLOTS, side, width), BF16),
        in_specs=[pl.BlockSpec(memory_space=pltpu.HBM)] * 4,
        out_specs=pl.BlockSpec(memory_space=pltpu.VMEM),
        scratch_shapes=[
            half,
            half,
            pltpu.SMEM((rows_dev, cols), I32),
            pltpu.VMEM(conv_weight.shape, BF16),
            pltpu.VMEM(conv_bias.shape, BF16),
            pltpu.VMEM((3 * 384, 256), BF16),
            pltpu.VMEM((chunks + 1, 48, LANES), F32),
            pltpu.VMEM((groups * side, 3 * 384), BF16),
            pltpu.VMEM((tiles + SHIFT_MOST, side, width), BF16),
            edge,
            edge,
            strip,
            strip,
            packed,
            packed,
            packed,
            packed,
            strip,
            strip,
            tile_pair,
            tile_pair,
            pltpu.VMEM((3, 32, LANES), F32),
            rim,
            rim,
            pltpu.VMEM((SHIFT_MOST, LANES), I32),
            pltpu.VMEM((SHIFT_MOST, LANES), I32),
            pltpu.VMEM((pair_size, LANES), I32),
            pltpu.VMEM((1, LANES), I32),
            pltpu.VMEM((1, LANES), I32),
            pltpu.SMEM((SLOTS,), I32),
            pltpu.SemaphoreType.DMA((5,)),
            pltpu.SemaphoreType.DMA((7,)),
            pltpu.SemaphoreType.DMA((7,)),
            pltpu.SemaphoreType.DMA((4,)),
        ],
        compiler_params=pltpu.CompilerParams(
            collective_id=0, has_side_effects=True, vmem_limit_bytes=24 * 1024 * 1024
        ),
        name="tissue_tiles",
    )(*(in_hbm(array) for array in (slide_pixels, tissue_mask, conv_weight, conv_bias)))


def solution(mesh):
    finer = Mesh(
        mesh.devices.reshape(mesh.shape["slides"], 4, 16, 2), ("slides", "row_0", "row_1", "row_2")
    )
    return jax.shard_map(
        on_device,
        mesh=finer,
        in_specs=(P(SLIDES_ROW, None), P(SLIDES_ROW, None), P(), P()),
        out_specs=P(SLIDES_ROW, None, None),
        check_vma=False,
    )
```

```python
import functools

import jax
import jax.numpy as jnp
from jax import lax
from jax.experimental import pallas as pl
from jax.experimental.pallas import tpu as pltpu
from jax.sharding import Mesh
from jax.sharding import PartitionSpec as P

SLOTS = 8
SHIFT_MOST = 2
ROW = ("row_0", "row_1", "row_2")
SLIDES_ROW = ("slides", "row_0", "row_1", "row_2")
MESH = pl.DeviceIdType.MESH
LANES = 128
F32 = jnp.float32
BF16 = jnp.bfloat16
I32 = jnp.int32


def kernel(
    pixels,
    mask_in,
    weight_in,
    bias_in,
    out,
    top_band,
    low_band,
    mask,
    weight,
    bias,
    big,
    fat,
    lhs,
    done,
    edge_first,
    edge_last,
    first_row,
    last_row,
    first_send,
    last_send,
    above_in,
    below_in,
    above,
    below,
    tile_send,
    tile_in,
    rim_work,
    rim_send,
    rim_in,
    note_send,
    note_in,
    counts,
    line_send,
    line_in,
    order,
    local_sem,
    send_sem,
    recv_sem,
    many_sem,
):
    x, z, c = (lax.axis_index(axis) for axis in ROW)
    planes, ring, cores = (lax.axis_size(axis) for axis in ROW)
    rows_dev, cols = mask_in.shape
    side = pixels.shape[0] // rows_dev
    tiles = rows_dev * cols
    chunks = pixels.shape[1] // (cols * LANES)
    groups = chunks // 2
    total = cols * chunks
    rank = (x * ring + z) * cores + c
    group_size = planes * ring * cores
    follows, leads = rank > 0, rank < group_size - 1
    early = (z < 2) & follows
    listens = (z == 0) & follows
    hub = (z == 0) & (c == 1)
    pair = x + 1 - 2 * (x % 2)

    def place(r):
        r = (r + group_size) % group_size
        return {"row_0": r // (ring * cores), "row_1": (r // cores) % ring, "row_2": r % cores}

    nxt, prv = place(rank + 1), place(rank - 1)

    def tell(where):
        pl.semaphore_signal(barrier, inc=1, device_id=where, device_id_type=MESH)

    barrier = pltpu.get_barrier_semaphore()
    bands = (top_band, low_band)
    copies = [
        pltpu.make_async_copy(mask_in, mask, local_sem.at[0]),
        pltpu.make_async_copy(pixels.at[side : 2 * side], low_band, local_sem.at[1]),
        pltpu.make_async_copy(pixels.at[0:side], top_band, local_sem.at[2]),
        pltpu.make_async_copy(weight_in, weight, local_sem.at[3]),
        pltpu.make_async_copy(bias_in, bias, local_sem.at[4]),
    ]
    for copy in (copies[1], copies[0], copies[3], copies[4]):
        copy.start()

    @pl.when(leads)
    def _():
        tell(nxt)

    @pl.when(follows)
    def _():
        tell(prv)

    @pl.when(listens)
    def _():
        def spread(k, _):
            for core in range(cores):
                there = (k == 0) & (core == c)

                @pl.when(jnp.logical_not(there))
                def _():
                    tell({"row_0": x, "row_1": k, "row_2": core})

                tell({"row_0": pair, "row_1": k, "row_2": core})
            return 0

        lax.fori_loop(0, ring, spread, 0)

    copies[0].wait()
    held = [mask[t // cols, t % cols] for t in range(tiles)]
    upto = []
    running = jnp.int32(0)
    for t in range(tiles):
        running = running + held[t]
        upto.append(running)
    own_count = running

    def nth(k):
        return sum(((upto[t] <= k).astype(I32) for t in range(tiles - 1)), jnp.int32(0))

    local = (x % 2) * (ring * cores) + z * cores + c
    counts[pl.ds(local, 1), :] = jnp.broadcast_to(own_count, (1, LANES))
    sent_tiles = [nth(own_count - SHIFT_MOST + a) for a in range(SHIFT_MOST)]
    for a in range(SHIFT_MOST):
        note_send[a : a + 1, :] = jnp.broadcast_to(sent_tiles[a], (1, LANES))
    def keep(row, col):
        inside = (col >= 0) & (col < cols)
        return jnp.where(inside, mask[row, jnp.clip(col, 0, cols - 1)], 0).astype(F32)

    lane = lax.broadcasted_iota(I32, (1, LANES), 1)
    lower = lane < LANES // 2

    def lanes_of(col, k):
        at = jnp.clip(col * chunks + k, 0, total - 1)
        return pl.ds(at * LANES, LANES)

    def outer_row(ref, send, row, block, pick):
        for col in range(cols):
            centre = held[row * cols + col].astype(F32)
            for k in range(chunks):
                at = col * chunks + k
                line = bands[row][block : block + 16, at * LANES : (at + 1) * LANES].astype(F32)
                ref[8 + at : 9 + at, :] = line[pick : pick + 1, :] * centre
        send[...] = ref[8 : 8 + total, :].astype(BF16)

    def stage(a):
        row, col = sent_tiles[a] // cols, sent_tiles[a] % cols
        row = row if a == 0 else rows_dev - 1

        def pixels_of(k):
            low = low_band[:, lanes_of(col, k)]
            return low if a else jnp.where(row == 0, top_band[:, lanes_of(col, k)], low)

        for k in range(chunks):
            tile_send[a, k] = pixels_of(k)
        right = pixels_of(chunks).astype(F32) * keep(row, col + 1)
        left = pixels_of(-1).astype(F32) * keep(row, col - 1)
        tile_send[a, chunks] = jnp.where(lower, right, left).astype(BF16)

    def one(source, pick):
        return source.astype(F32)[pick : pick + 1, :]

    def inner_rim(row, pick, block, col):
        centre = keep(row, col)
        for k in range(chunks):
            yield one(bands[row][block : block + 16, lanes_of(col, k)], pick) * centre
        right = one(bands[row][block : block + 16, lanes_of(col, chunks)], pick) * keep(row, col + 1)
        left = one(bands[row][block : block + 16, lanes_of(col, -1)], pick) * keep(row, col - 1)
        yield jnp.where(lower, right, left)

    def edge_rim(ref, col):
        step = col * (chunks // 8) + 1
        body = ref[pl.ds(step * 8, chunks), :]
        for k in range(chunks):
            yield body[k : k + 1, :]
        left = ref[pl.ds((step - 1) * 8, 8), :][7:8, :]
        right = ref[pl.ds((step + chunks // 8) * 8, 8), :][0:1, :]
        yield jnp.where(lower, right, left)

    def build_big():
        copies[3].wait()
        copies[4].wait()
        nothing = jnp.zeros((64, 64), BF16)
        for dy in range(3):
            taps = [weight[dy, dx] for dx in range(3)]
            for p in (0, 1, 2, 3, 4, -1):
                parts = [taps[p - q + 1] if 0 <= p - q + 1 < 3 else nothing for q in range(4)]
                at = dy * 384 + (p if p >= 0 else 5) * 64
                big[at : at + 64, :] = jnp.concatenate(parts, axis=1)

    def bias_row():
        short = bias[...].astype(F32).reshape(1, 64)
        return jnp.concatenate([short] * 4, axis=1)

    def multiply():
        for dy in range(3):
            rows = slice(7 + dy, 7 + dy + side)
            for g in range(groups):
                at = slice(g * side, (g + 1) * side)
                right = fat[2 * g + 2 if g < groups - 1 else chunks, rows, :]
                left = fat[2 * g - 1 if g > 0 else chunks, rows, :]
                lhs[at, dy * 384 : dy * 384 + 128] = fat[2 * g, rows, :].astype(BF16)
                lhs[at, dy * 384 + 128 : dy * 384 + 256] = fat[2 * g + 1, rows, :].astype(BF16)
                lhs[at, dy * 384 + 256 : dy * 384 + 384] = jnp.where(lower, right, left).astype(BF16)
        return jnp.dot(lhs[...], big[...], preferred_element_type=F32) + bias_row()

    def finish(result, slot):
        for g in range(groups):
            done[slot, :, g * 256 : (g + 1) * 256] = result[g * side : (g + 1) * side].astype(BF16)

    def own_tiles():
        build_big()
        for row in range(rows_dev):

            def tile(col, _, row=row):
                band = bands[row]
                for k in range(chunks):
                    fat[k, 8 : 8 + side, :] = band[:, lanes_of(col, k)].astype(F32)
                right = band[:, lanes_of(col, chunks)].astype(F32) * keep(row, col + 1)
                left = band[:, lanes_of(col, -1)].astype(F32) * keep(row, col - 1)
                fat[chunks, 8 : 8 + side, :] = jnp.where(lower, right, left)
                if row == 0:
                    rim = inner_rim(1, 0, 0, col)
                    for k, line in enumerate(rim):
                        fat[k, 7:8, :] = jnp.zeros((1, LANES), F32)
                        fat[k, 8 + side : 9 + side, :] = line
                else:
                    rim = inner_rim(0, 15, side - 16, col)
                    for k, line in enumerate(rim):
                        fat[k, 7:8, :] = line
                        fat[k, 8 + side : 9 + side, :] = jnp.zeros((1, LANES), F32)
                result = multiply()
                finish(result, row * cols + col)
                for g in range(groups):
                    if row == 0:
                        edge_first[col, g : g + 1, :] = result[g * side : g * side + 1]
                    else:
                        edge_last[col, g : g + 1, :] = result[(g + 1) * side - 1 : (g + 1) * side]
                return 0

            lax.fori_loop(0, cols, tile, 0)

    def remote(source, target, k, where):
        return pltpu.make_async_remote_copy(
            source, target, send_sem.at[k], recv_sem.at[k], device_id=where, device_id_type=MESH
        )

    mine = counts.at[pl.ds(local, 1)]

    def count_to(plane, core):
        return pltpu.make_async_remote_copy(
            mine, mine, many_sem.at[0], many_sem.at[1],
            device_id={"row_0": plane, "row_1": 0, "row_2": core}, device_id_type=MESH,
        )

    hearers = [
        (plane, core, (((plane > 0) | (core > 0)) & jnp.logical_not(here & (z == 0) & (c == core))))
        for plane, here in ((x, True), (pair, False))
        for core in range(2)
    ]

    def arrive():
        others = sum((used.astype(I32) for _, _, used in hearers), jnp.int32(0))
        pl.semaphore_wait(barrier, others + follows.astype(I32) + leads.astype(I32))
        for plane, core, used in hearers:

            @pl.when(used)
            def _(plane=plane, core=core):
                count_to(plane, core).start()

    note = remote(note_send, note_in, 0, nxt)
    down = remote(last_send, above_in, 1, nxt)
    up = remote(first_send, below_in, 2, prv)
    bodies = [remote(tile_send.at[a], tile_in.at[a], 3 + a, nxt) for a in range(SHIFT_MOST)]
    fixed_rims = remote(rim_send.at[0:2], rim_in.at[0:2], 5, nxt)
    last_rim = remote(rim_send.at[2], rim_in.at[2], 6, nxt)
    def send_low():
        @pl.when(leads)
        def _():
            note.start()
            bodies[1].start()
            down.start()

    def send_top():
        stage(0)
        inner_rims()

        @pl.when(leads)
        def _():
            fixed_rims.start()
            bodies[0].start()

        outer_row(first_row, first_send, 0, 0, 0)

        @pl.when(follows)
        def _():
            up.start()

    def inner_rims():
        for k, line in enumerate(inner_rim(1, 0, 0, sent_tiles[0] % cols)):
            rim_work[0, k : k + 1, :] = line
        for k, line in enumerate(inner_rim(0, 15, side - 16, sent_tiles[1] % cols)):
            rim_work[1, k : k + 1, :] = line
        rim_send[0:2] = rim_work[0:2].astype(BF16)

    def send_last_rim():
        @pl.when(follows)
        def _():
            down.wait_recv()
            above[8 : 8 + total, :] = above_in[...].astype(F32)

        @pl.when(jnp.logical_not(follows))
        def _():
            above[8 : 8 + total, :] = jnp.zeros((total, LANES), F32)

        row, col = sent_tiles[0] // cols, sent_tiles[0] % cols
        for k, (outer, inner) in enumerate(zip(edge_rim(above, col), inner_rim(0, 15, side - 16, col))):
            rim_work[2, k : k + 1, :] = jnp.where(row == 0, outer, inner)
        rim_send[2] = rim_work[2].astype(BF16)

        @pl.when(leads)
        def _():
            last_rim.start()

    zeros8 = jnp.zeros((8, LANES), F32)
    for ref in (first_row, last_row, above, below):
        ref[0:8, :] = zeros8
        ref[8 + total : 16 + total, :] = zeros8

    @pl.when(jnp.logical_not(early))
    def _():
        arrive()

    copies[1].wait()
    copies[2].start()
    stage(1)
    outer_row(last_row, last_send, rows_dev - 1, side - 16, 15)

    @pl.when(early)
    def _():
        copies[2].wait()
        own_tiles()
        arrive()
        send_low()
        send_top()

    @pl.when(jnp.logical_not(early))
    def _():
        send_low()
        copies[2].wait()
        send_top()
        send_last_rim()
        own_tiles()

    for k in range(SLOTS):
        order[k] = nth(jnp.int32(k))

    @pl.when(leads)
    def _():
        up.wait_recv()
        below[8 : 8 + total, :] = below_in[...].astype(F32)

    @pl.when(jnp.logical_not(leads))
    def _():
        below[8 : 8 + total, :] = jnp.zeros((total, LANES), F32)

    def join(ref, edge, dy, row, block, pick):
        half = total // 2
        even = ref[pl.ds(8, half, 2), :]
        odd = ref[pl.ds(9, half, 2), :]
        right = ref[pl.ds(10, half, 2), :]
        left = ref[pl.ds(7, half, 2), :]
        side_by = jnp.concatenate([even, odd, jnp.where(lower, right, left)], axis=1).astype(BF16)
        more = jnp.dot(side_by, big[dy * 384 : (dy + 1) * 384, :], preferred_element_type=F32)
        at_row = lax.broadcasted_iota(I32, (16, 256), 0) == pick
        for col in range(cols):
            whole = more[col * groups : (col + 1) * groups] + edge[col]
            for g in range(groups):
                span = slice(g * 256, (g + 1) * 256)
                old = done[row * cols + col, block : block + 16, span].astype(F32)
                new = jnp.where(at_row, whole[g : g + 1, :], old)
                done[row * cols + col, block : block + 16, span] = new.astype(BF16)

    join(below, edge_last, 2, rows_dev - 1, side - 16, 15)

    @pl.when(early)
    def _():
        send_last_rim()

    join(above, edge_first, 0, 0, 0, 0)

    def taken(a):
        came = jnp.max(note_in[a : a + 1, :])
        row, col = came // cols, came % cols
        bodies[a].wait_recv()
        for k in range(chunks + 1):
            fat[k, 8 : 8 + side, :] = tile_in[a, k].astype(F32)
        over = rim_in[1 if a else 2].astype(F32)
        under = rim_in[0].astype(F32)
        for k, line in enumerate(edge_rim(first_row, col)):
            fat[k, 7:8, :] = over[k : k + 1, :]
            if a == 0:
                line = jnp.where(row == rows_dev - 1, line, under[k : k + 1, :])
            fat[k, 8 + side : 9 + side, :] = line
        finish(multiply(), tiles + a)

    @pl.when(follows)
    def _():
        note.wait_recv()
        fixed_rims.wait_recv()
        taken(1)

    @pl.when(listens)
    def _():
        others = counts.at[pl.ds(0, 2 * ring * cores - 1)]
        pltpu.make_async_copy(others, others, many_sem.at[1]).wait()
        table = counts[...]
        spot = lax.broadcasted_iota(I32, table.shape, 0) == lax.broadcasted_iota(I32, table.shape, 1)
        line_send[...] = jnp.sum(jnp.where(spot, table, 0), axis=0, keepdims=True)

    @pl.when(hub)
    def _():
        def spread(k, _):
            for core in range(2):
                pltpu.make_async_remote_copy(
                    line_send, line_in, many_sem.at[2], many_sem.at[3],
                    device_id={"row_0": x, "row_1": k, "row_2": core}, device_id_type=MESH,
                ).start()
            return 0

        lax.fori_loop(1, ring, spread, 0)

    @pl.when(z > 0)
    def _():
        pltpu.make_async_copy(line_in, line_in, many_sem.at[3]).wait()

    @pl.when(jnp.logical_not(follows))
    def _():
        line_in[...] = jnp.zeros(line_in.shape, I32)

    line = jnp.where(listens, line_send[...], line_in[...])
    before = jnp.sum(jnp.where(lane < local, line, 0))
    whole = jnp.sum(line)
    start = jnp.where(x < planes // 2, 0, SLOTS * ring * cores * 2 - whole)
    excess = jnp.clip(start + before - SLOTS * local, 0, SHIFT_MOST)

    def fill(j):
        own = order[jnp.clip(j - excess, 0, SLOTS - 1)]
        came = tiles + SHIFT_MOST - excess + j
        out[j] = done[jnp.clip(jnp.where(j < excess, came, own), 0, tiles + SHIFT_MOST - 1)]

    for j in range(SHIFT_MOST, SLOTS):
        fill(j)

    @pl.when(follows)
    def _():
        last_rim.wait_recv()
        taken(0)

    for j in range(SHIFT_MOST):
        fill(j)

    @pl.when(leads)
    def _():
        for copy in (note, down, *bodies, fixed_rims, last_rim):
            copy.wait_send()

    @pl.when(follows)
    def _():
        up.wait_send()

    for plane, core, used in hearers:

        @pl.when(used)
        def _(plane=plane, core=core):
            count_to(plane, core).wait_send()

    @pl.when(hub)
    def _():
        sent = counts.at[pl.ds(0, (ring - 1) * cores)]
        pltpu.make_async_copy(sent, sent, many_sem.at[2]).wait()


def in_hbm(array):
    return pltpu.with_memory_space_constraint(array, pltpu.HBM)


def on_device(slide_pixels, tissue_mask, conv_weight, conv_bias):
    rows_dev, cols = tissue_mask.shape
    side = slide_pixels.shape[0] // rows_dev
    width = slide_pixels.shape[1] // cols
    chunks = width // LANES
    groups = chunks // 2
    total = cols * chunks
    tiles = rows_dev * cols
    pair_size = 2 * lax.axis_size("row_1") * lax.axis_size("row_2")
    half = pltpu.VMEM((side, slide_pixels.shape[1]), BF16)
    strip = pltpu.VMEM((total + 16, LANES), F32)
    packed = pltpu.VMEM((total, LANES), BF16)
    rim = pltpu.VMEM((3, 32, LANES), BF16)
    tile_pair = pltpu.VMEM((SHIFT_MOST, chunks + 1, side, LANES), BF16)
    edge = pltpu.VMEM((cols, groups, 256), F32)
    return pl.pallas_call(
        kernel,
        out_shape=pltpu.VMEM((SLOTS, side, width), BF16),
        in_specs=[pl.BlockSpec(memory_space=pltpu.HBM)] * 4,
        out_specs=pl.BlockSpec(memory_space=pltpu.VMEM),
        scratch_shapes=[
            half,
            half,
            pltpu.SMEM((rows_dev, cols), I32),
            pltpu.VMEM(conv_weight.shape, BF16),
            pltpu.VMEM(conv_bias.shape, BF16),
            pltpu.VMEM((3 * 384, 256), BF16),
            pltpu.VMEM((chunks + 1, 48, LANES), F32),
            pltpu.VMEM((groups * side, 3 * 384), BF16),
            pltpu.VMEM((tiles + SHIFT_MOST, side, width), BF16),
            edge,
            edge,
            strip,
            strip,
            packed,
            packed,
            packed,
            packed,
            strip,
            strip,
            tile_pair,
            tile_pair,
            pltpu.VMEM((3, 32, LANES), F32),
            rim,
            rim,
            pltpu.VMEM((SHIFT_MOST, LANES), I32),
            pltpu.VMEM((SHIFT_MOST, LANES), I32),
            pltpu.VMEM((pair_size, LANES), I32),
            pltpu.VMEM((1, LANES), I32),
            pltpu.VMEM((1, LANES), I32),
            pltpu.SMEM((SLOTS,), I32),
            pltpu.SemaphoreType.DMA((5,)),
            pltpu.SemaphoreType.DMA((7,)),
            pltpu.SemaphoreType.DMA((7,)),
            pltpu.SemaphoreType.DMA((4,)),
        ],
        compiler_params=pltpu.CompilerParams(
            collective_id=0, has_side_effects=True, vmem_limit_bytes=24 * 1024 * 1024
        ),
        name="tissue_tiles",
    )(*(in_hbm(array) for array in (slide_pixels, tissue_mask, conv_weight, conv_bias)))


def solution(mesh):
    finer = Mesh(
        mesh.devices.reshape(mesh.shape["slides"], 4, 16, 2), ("slides", "row_0", "row_1", "row_2")
    )
    return jax.shard_map(
        on_device,
        mesh=finer,
        in_specs=(P(SLIDES_ROW, None), P(SLIDES_ROW, None), P(), P()),
        out_specs=P(SLIDES_ROW, None, None),
        check_vma=False,
    )
```

```python
import functools

import jax
import jax.numpy as jnp
from jax import lax
from jax.experimental import pallas as pl
from jax.experimental.pallas import tpu as pltpu
from jax.sharding import Mesh
from jax.sharding import PartitionSpec as P

SLOTS = 8
SHIFT_MOST = 2
ROW = ("row_0", "row_1", "row_2")
SLIDES_ROW = ("slides", "row_0", "row_1", "row_2")
MESH = pl.DeviceIdType.MESH
LANES = 128
F32 = jnp.float32
BF16 = jnp.bfloat16
I32 = jnp.int32


def kernel(
    pixels,
    mask_in,
    weight_in,
    bias_in,
    out,
    top_band,
    low_band,
    mask,
    weight,
    bias,
    big,
    fat,
    lhs,
    done,
    edge_first,
    edge_last,
    first_row,
    last_row,
    first_send,
    last_send,
    above_in,
    below_in,
    above,
    below,
    tile_send,
    tile_in,
    rim_work,
    rim_send,
    rim_in,
    note_send,
    note_in,
    counts,
    line_send,
    line_in,
    order,
    excess,
    local_sem,
    send_sem,
    recv_sem,
    many_sem,
):
    x, z, c = (lax.axis_index(axis) for axis in ROW)
    planes, ring, cores = (lax.axis_size(axis) for axis in ROW)
    rows_dev, cols = mask_in.shape
    side = pixels.shape[0] // rows_dev
    tiles = rows_dev * cols
    chunks = pixels.shape[1] // (cols * LANES)
    groups = chunks // 2
    total = cols * chunks
    rank = (x * ring + z) * cores + c
    local = (x % 2) * (ring * cores) + z * cores + c
    group_size = planes * ring * cores
    follows, leads = rank > 0, rank < group_size - 1
    early = (z < 2) & follows
    hub = (z == 1) & (c == 1)
    inner = x > 0
    listens = (c == 1) & (z == 1 - inner.astype(I32))
    pair = x + 1 - 2 * (x % 2)

    def place(r):
        r = (r + group_size) % group_size
        return {"row_0": r // (ring * cores), "row_1": (r // cores) % ring, "row_2": r % cores}

    nxt, prv = place(rank + 1), place(rank - 1)

    def tell(where):
        pl.semaphore_signal(barrier, inc=1, device_id=where, device_id_type=MESH)

    barrier = pltpu.get_barrier_semaphore()
    bands = (top_band, low_band)
    copies = [
        pltpu.make_async_copy(mask_in, mask, local_sem.at[0]),
        pltpu.make_async_copy(pixels.at[side : 2 * side - 16], low_band.at[0 : side - 16], local_sem.at[2]),
        pltpu.make_async_copy(pixels.at[0:side], top_band, local_sem.at[0]),
        pltpu.make_async_copy(weight_in, weight, local_sem.at[1]),
        pltpu.make_async_copy(bias_in, bias, local_sem.at[2]),
        pltpu.make_async_copy(pixels.at[2 * side - 16 : 2 * side], low_band.at[side - 16 : side], local_sem.at[1]),
    ]
    for copy in (copies[0], copies[5], copies[1]):
        copy.start()

    @pl.when(leads)
    def _():
        tell(nxt)

    @pl.when(follows)
    def _():
        tell(prv)

    @pl.when(listens)
    def _():
        def spread(k, _):
            for core in range(cores):
                there = (k == z) & (core == c)

                @pl.when(jnp.logical_not(there))
                def _():
                    tell({"row_0": x, "row_1": k, "row_2": core})

                tell({"row_0": pair, "row_1": k, "row_2": core})
            return 0

        lax.fori_loop(0, ring, spread, 0)

    copies[0].wait()
    held = [mask[t // cols, t % cols] for t in range(tiles)]
    def keep(row, col):
        inside = (col >= 0) & (col < cols)
        return jnp.where(inside, mask[row, jnp.clip(col, 0, cols - 1)], 0).astype(F32)

    lane = lax.broadcasted_iota(I32, (1, LANES), 1)
    lower = lane < LANES // 2

    def lanes_of(col, k):
        at = jnp.clip(col * chunks + k, 0, total - 1)
        return pl.ds(at * LANES, LANES)

    def outer_row(ref, send, row, block, pick):
        for col in range(cols):
            centre = held[row * cols + col].astype(F32)
            for k in range(chunks):
                at = col * chunks + k
                line = bands[row][block : block + 16, at * LANES : (at + 1) * LANES].astype(F32)
                ref[8 + at : 9 + at, :] = line[pick : pick + 1, :] * centre
        send[...] = ref[8 : 8 + total, :].astype(BF16)

    def stage(a):
        row, col = sent_tiles[a] // cols, sent_tiles[a] % cols
        row = row if a == 0 else rows_dev - 1

        def pixels_of(k):
            low = low_band[:, lanes_of(col, k)]
            return low if a else jnp.where(row == 0, top_band[:, lanes_of(col, k)], low)

        for k in range(chunks):
            tile_send[a, k + 1] = pixels_of(k)
        right = pixels_of(chunks).astype(F32) * keep(row, col + 1)
        left = pixels_of(-1).astype(F32) * keep(row, col - 1)
        tile_send[a, 0] = jnp.where(lower, right, left).astype(BF16)

    def one(source, pick):
        return source.astype(F32)[pick : pick + 1, :]

    def inner_rim(row, pick, block, col):
        centre = keep(row, col)
        for k in range(chunks):
            yield one(bands[row][block : block + 16, lanes_of(col, k)], pick) * centre
        right = one(bands[row][block : block + 16, lanes_of(col, chunks)], pick) * keep(row, col + 1)
        left = one(bands[row][block : block + 16, lanes_of(col, -1)], pick) * keep(row, col - 1)
        yield jnp.where(lower, right, left)

    def edge_rim(ref, col):
        step = col * (chunks // 8) + 1
        body = ref[pl.ds(step * 8, chunks), :]
        for k in range(chunks):
            yield body[k : k + 1, :]
        left = ref[pl.ds((step - 1) * 8, 8), :][7:8, :]
        right = ref[pl.ds((step + chunks // 8) * 8, 8), :][0:1, :]
        yield jnp.where(lower, right, left)

    def build_big():
        copies[3].wait()
        copies[4].wait()
        nothing = jnp.zeros((64, 64), BF16)
        for dy in range(3):
            taps = [weight[dy, dx] for dx in range(3)]
            for p in (0, 1, 2, 3, 4, -1):
                parts = [taps[p - q + 1] if 0 <= p - q + 1 < 3 else nothing for q in range(4)]
                at = dy * 384 + (p if p >= 0 else 5) * 64
                big[at : at + 64, :] = jnp.concatenate(parts, axis=1)

    def bias_row():
        short = bias[...].astype(F32).reshape(1, 64)
        return jnp.concatenate([short] * 4, axis=1)

    def multiply(first=0, last=groups):
        for dy in range(3):
            rows = slice(7 + dy, 7 + dy + side)
            for g in range(first, last):
                at = slice((g - first) * side, (g - first + 1) * side)
                right = fat[2 * g + 2 if g < groups - 1 else chunks, rows, :]
                left = fat[2 * g - 1 if g > 0 else chunks, rows, :]
                lhs[at, dy * 384 : dy * 384 + 128] = fat[2 * g, rows, :].astype(BF16)
                lhs[at, dy * 384 + 128 : dy * 384 + 256] = fat[2 * g + 1, rows, :].astype(BF16)
                lhs[at, dy * 384 + 256 : dy * 384 + 384] = jnp.where(lower, right, left).astype(BF16)
        used = lhs[0 : (last - first) * side]
        return jnp.dot(used, big[...], preferred_element_type=F32) + bias_row()

    def finish(result, slot, first=0, last=groups):
        for g in range(first, last):
            part = result[(g - first) * side : (g - first + 1) * side]
            done[slot, :, g * 256 : (g + 1) * 256] = part.astype(BF16)

    def own_tiles():
        build_big()
        for row in range(rows_dev):

            def tile(col, _, row=row):
                band = bands[row]
                for k in range(chunks):
                    fat[k, 8 : 8 + side, :] = band[:, lanes_of(col, k)].astype(F32)
                right = band[:, lanes_of(col, chunks)].astype(F32) * keep(row, col + 1)
                left = band[:, lanes_of(col, -1)].astype(F32) * keep(row, col - 1)
                fat[chunks, 8 : 8 + side, :] = jnp.where(lower, right, left)
                if row == 0:
                    rim = inner_rim(1, 0, 0, col)
                    for k, line in enumerate(rim):
                        fat[k, 7:8, :] = jnp.zeros((1, LANES), F32)
                        fat[k, 8 + side : 9 + side, :] = line
                else:
                    rim = inner_rim(0, 15, side - 16, col)
                    for k, line in enumerate(rim):
                        fat[k, 7:8, :] = line
                        fat[k, 8 + side : 9 + side, :] = jnp.zeros((1, LANES), F32)
                result = multiply()
                finish(result, row * cols + col)
                for g in range(groups):
                    if row == 0:
                        edge_first[col, g : g + 1, :] = result[g * side : g * side + 1]
                    else:
                        edge_last[col, g : g + 1, :] = result[(g + 1) * side - 1 : (g + 1) * side]
                return 0

            lax.fori_loop(0, cols, tile, 0)

    def remote(source, target, sent, came, where):
        return pltpu.make_async_remote_copy(
            source, target, send_sem.at[sent], recv_sem.at[came], device_id=where, device_id_type=MESH
        )

    mine = counts.at[pl.ds(local, 1)]

    def count_to(plane):
        level = 1 - (plane > 0).astype(I32)
        return pltpu.make_async_remote_copy(
            mine, mine, many_sem.at[0], many_sem.at[1],
            device_id={"row_0": plane, "row_1": level, "row_2": 1}, device_id_type=MESH,
        )

    hearers = [(x, jnp.logical_not(listens)), (pair, listens | jnp.logical_not(listens))]

    def arrive():
        others = 2 - listens.astype(I32)
        pl.semaphore_wait(barrier, others + follows.astype(I32) + leads.astype(I32))

    def send_counts():
        for spot, used in hearers:

            @pl.when(used)
            def _(spot=spot):
                count_to(spot).start()

    note = remote(note_send, note_in, 0, 0, nxt)
    down = remote(last_send, above_in, 1, 1, nxt)
    up = remote(first_send, below_in, 2, 2, prv)
    cut = chunks // 2 + 2
    pieces = ((slice(0, cut), slice(cut, chunks + 1)), (slice(0, chunks + 1),))
    bodies = [
        [remote(tile_send.at[a, piece], tile_in.at[a, piece], 3, 4 + i - a, nxt) for i, piece in enumerate(pieces[a])]
        for a in range(SHIFT_MOST)
    ]
    rims = remote(rim_send, rim_in, 4, 6, nxt)

    def send_halo():
        @pl.when(leads)
        def _():
            down.start()

    def low_tile():
        copies[1].wait()
        for copy in copies[2:5]:
            copy.start()
        stage(1)

    def send_low():
        @pl.when(leads)
        def _():
            note.start()
            bodies[1][0].start()

    def send_top():
        stage(0)
        inner_rims()

        @pl.when(jnp.logical_not(early))
        def _():
            send_last_rim()

        @pl.when(leads)
        def _():
            bodies[0][0].start()
            bodies[0][1].start()

        outer_row(first_row, first_send, 0, 0, 0)

        @pl.when(follows)
        def _():
            up.start()

    def rim_row(rim, k):
        return rim * chunks + k if k < chunks else 3 * chunks + rim

    def set_rim(rim, k, line):
        at = rim_row(rim, k)
        rim_work[at : at + 1, :] = line

    def inner_rims():
        for k, line in enumerate(inner_rim(1, 0, 0, sent_tiles[0] % cols)):
            set_rim(0, k, line)
        for k, line in enumerate(inner_rim(0, 15, side - 16, sent_tiles[1] % cols)):
            set_rim(1, k, line)

    def send_last_rim():
        @pl.when(follows)
        def _():
            down.wait_recv()
            above[8 : 8 + total, :] = above_in[...].astype(F32)

        @pl.when(jnp.logical_not(follows))
        def _():
            above[8 : 8 + total, :] = jnp.zeros((total, LANES), F32)

        row, col = sent_tiles[0] // cols, sent_tiles[0] % cols
        for k, (outer, inner) in enumerate(zip(edge_rim(above, col), inner_rim(0, 15, side - 16, col))):
            set_rim(2, k, jnp.where(row == 0, outer, inner))
        rim_send[...] = rim_work[...].astype(BF16)

        @pl.when(leads)
        def _():
            rims.start()

    copies[5].wait()
    outer_row(last_row, last_send, rows_dev - 1, side - 16, 15)

    @pl.when(jnp.logical_not(early))
    def _():
        arrive()
        send_halo()

    upto = []
    running = jnp.int32(0)
    for t in range(tiles):
        running = running + held[t]
        upto.append(running)
    own_count = running

    def nth(k):
        return sum(((upto[t] <= k).astype(I32) for t in range(tiles - 1)), jnp.int32(0))

    counts[pl.ds(local, 1), :] = jnp.broadcast_to(own_count, (1, LANES))
    sent_tiles = [nth(own_count - SHIFT_MOST + a) for a in range(SHIFT_MOST)]
    for a in range(SHIFT_MOST):
        note_send[a : a + 1, :] = jnp.broadcast_to(sent_tiles[a], (1, LANES))
    note_send[SHIFT_MOST : SHIFT_MOST + 1, :] = jnp.broadcast_to(own_count, (1, LANES))
    zeros8 = jnp.zeros((8, LANES), F32)
    for ref in (first_row, above, below):
        ref[0:8, :] = zeros8
        ref[8 + total : 16 + total, :] = zeros8

    @pl.when(early)
    def _():
        low_tile()
        copies[2].wait()
        own_tiles()
        arrive()
        send_counts()
        send_halo()
        send_low()
        send_top()

    @pl.when(jnp.logical_not(early))
    def _():
        send_counts()
        low_tile()
        send_low()
        copies[2].wait()
        send_top()
        own_tiles()

    for k in range(SLOTS):
        order[k] = nth(jnp.int32(k))

    @pl.when(leads)
    def _():
        up.wait_recv()
        below[8 : 8 + total, :] = below_in[...].astype(F32)

    @pl.when(jnp.logical_not(leads))
    def _():
        below[8 : 8 + total, :] = jnp.zeros((total, LANES), F32)

    def join(ref, edge, dy, row, block, pick):
        half = total // 2
        even = ref[pl.ds(8, half, 2), :]
        odd = ref[pl.ds(9, half, 2), :]
        right = ref[pl.ds(10, half, 2), :]
        left = ref[pl.ds(7, half, 2), :]
        side_by = jnp.concatenate([even, odd, jnp.where(lower, right, left)], axis=1).astype(BF16)
        more = jnp.dot(side_by, big[dy * 384 : (dy + 1) * 384, :], preferred_element_type=F32)
        at_row = lax.broadcasted_iota(I32, (16, 256), 0) == pick
        for col in range(cols):
            whole = more[col * groups : (col + 1) * groups] + edge[col]
            for g in range(groups):
                span = slice(g * 256, (g + 1) * 256)
                old = done[row * cols + col, block : block + 16, span].astype(F32)
                new = jnp.where(at_row, whole[g : g + 1, :], old)
                done[row * cols + col, block : block + 16, span] = new.astype(BF16)

    join(below, edge_last, 2, rows_dev - 1, side - 16, 15)

    @pl.when(early)
    def _():
        send_last_rim()

    join(above, edge_first, 0, 0, 0, 0)

    def taken(a):
        came = jnp.max(note_in[a : a + 1, :])
        row, col = came // cols, came % cols
        came_rims = rim_in[...].astype(F32)

        def rim(which, k):
            at = rim_row(which, k)
            return came_rims[at : at + 1, :]

        for k, line in enumerate(edge_rim(first_row, col)):
            fat[k, 7:8, :] = rim(1 if a else 2, k)
            if a == 0:
                line = jnp.where(row == rows_dev - 1, line, rim(0, k))
            fat[k, 8 + side : 9 + side, :] = line
        for i, piece in enumerate(pieces[a]):
            bodies[a][i].wait_recv()
            for k in range(piece.start, piece.stop):
                fat[k - 1 if k else chunks, 8 : 8 + side, :] = tile_in[a, k].astype(F32)
            parts = len(pieces[a])
            span = (i * groups // parts, (i + 1) * groups // parts)
            result = multiply(*span)
            if a:
                finish(result, tiles, *span)
            else:
                lead_slot(result, *span)

    def lead_slot(result, first, last):
        for g in range(first, last):
            part = result[(g - first) * side : (g - first + 1) * side].astype(BF16)
            lanes = slice(g * 256, (g + 1) * 256)
            out[0, :, lanes] = jnp.where(excess[0] == SHIFT_MOST, part, out[0, :, lanes])

    @pl.when(leads)
    def _():
        for copy in (note, down, rims):
            copy.wait_send()
        pltpu.make_async_copy(tile_send, tile_send, send_sem.at[3]).wait()

    @pl.when(follows)
    def _():
        up.wait_send()

    for spot, used in hearers:

        @pl.when(used)
        def _(spot=spot):
            count_to(spot).wait_send()

    def settle(line):
        before = jnp.sum(jnp.where(lane < local, line, 0))
        whole = jnp.sum(line)
        start = jnp.where(x < planes // 2, 0, SLOTS * ring * cores * 2 - whole)
        excess[0] = jnp.clip(start + before - SLOTS * local, 0, SHIFT_MOST)

    @pl.when(follows)
    def _():
        note.wait_recv()

    @pl.when(listens)
    def _():
        others = counts.at[pl.ds(0, 2 * ring * cores - 1)]
        pltpu.make_async_copy(others, others, many_sem.at[1]).wait()
        table = counts[...]
        spot = lax.broadcasted_iota(I32, table.shape, 0) == lax.broadcasted_iota(I32, table.shape, 1)
        line = jnp.sum(jnp.where(spot, table, 0), axis=0, keepdims=True)
        line_send[...] = line
        settle(line)

    def line_to(source, level, core):
        return pltpu.make_async_remote_copy(
            source, line_in, many_sem.at[0], many_sem.at[2],
            device_id={"row_0": x, "row_1": level, "row_2": core}, device_id_type=MESH,
        )

    @pl.when(listens & inner)
    def _():
        line_to(line_send, 0, 0).start()
        line_to(line_send, 1, 1).start()

    @pl.when(hub & jnp.logical_not(inner))
    def _():
        line_in[...] = line_send[...]

    def hear():
        pltpu.make_async_copy(line_in, line_in, many_sem.at[2]).wait()
        settle(line_in[...])

    @pl.when((z == 0) & (c == 0) & inner)
    def _():
        hear()

    @pl.when(follows)
    def _():
        rims.wait_recv()
        taken(1)

    @pl.when((z > 0) & (inner | jnp.logical_not(hub)))
    def _():
        hear()

    @pl.when(hub)
    def _():
        def spread(k, _):
            for core in range(2):
                line_to(line_in, k, core).start()
            return 0

        line_to(line_in, 1, 0).start()
        lax.fori_loop(2, ring, spread, 0)

    @pl.when(rank == 0)
    def _():
        excess[0] = jnp.int32(0)

    @pl.when(rank == 1)
    def _():
        beside = jnp.max(note_in[SHIFT_MOST : SHIFT_MOST + 1, :])
        excess[0] = jnp.clip(beside - SLOTS, 0, SHIFT_MOST)

    shift = excess[0]

    for j in range(SLOTS):
        own = order[jnp.clip(j - shift, 0, SLOTS - 1)]
        out[j] = done[jnp.where(j == shift - 1, tiles, own)]

    @pl.when(follows)
    def _():
        taken(0)

    @pl.when(listens & inner)
    def _():
        both = counts.at[pl.ds(0, 2)]
        pltpu.make_async_copy(both, both, many_sem.at[0]).wait()

    @pl.when(hub)
    def _():
        sent = counts.at[pl.ds(0, (ring - 1) * cores - 1)]
        pltpu.make_async_copy(sent, sent, many_sem.at[0]).wait()


def in_hbm(array):
    return pltpu.with_memory_space_constraint(array, pltpu.HBM)


def on_device(slide_pixels, tissue_mask, conv_weight, conv_bias):
    rows_dev, cols = tissue_mask.shape
    side = slide_pixels.shape[0] // rows_dev
    width = slide_pixels.shape[1] // cols
    chunks = width // LANES
    groups = chunks // 2
    total = cols * chunks
    tiles = rows_dev * cols
    pair_size = 2 * lax.axis_size("row_1") * lax.axis_size("row_2")
    half = pltpu.VMEM((side, slide_pixels.shape[1]), BF16)
    strip = pltpu.VMEM((total + 16, LANES), F32)
    packed = pltpu.VMEM((total, LANES), BF16)
    rim = pltpu.VMEM((4 * chunks, LANES), BF16)
    tile_pair = pltpu.VMEM((SHIFT_MOST, chunks + 1, side, LANES), BF16)
    edge = pltpu.VMEM((cols, groups, 256), F32)
    return pl.pallas_call(
        kernel,
        out_shape=pltpu.VMEM((SLOTS, side, width), BF16),
        in_specs=[pl.BlockSpec(memory_space=pltpu.HBM)] * 4,
        out_specs=pl.BlockSpec(memory_space=pltpu.VMEM),
        scratch_shapes=[
            half,
            half,
            pltpu.SMEM((rows_dev, cols), I32),
            pltpu.VMEM(conv_weight.shape, BF16),
            pltpu.VMEM(conv_bias.shape, BF16),
            pltpu.VMEM((3 * 384, 256), BF16),
            pltpu.VMEM((chunks + 1, 48, LANES), F32),
            pltpu.VMEM((groups * side, 3 * 384), BF16),
            pltpu.VMEM((tiles + 1, side, width), BF16),
            edge,
            edge,
            strip,
            strip,
            packed,
            packed,
            packed,
            packed,
            strip,
            strip,
            tile_pair,
            tile_pair,
            pltpu.VMEM((4 * chunks, LANES), F32),
            rim,
            rim,
            pltpu.VMEM((SHIFT_MOST + 1, LANES), I32),
            pltpu.VMEM((SHIFT_MOST + 1, LANES), I32),
            pltpu.VMEM((pair_size, LANES), I32),
            pltpu.VMEM((1, LANES), I32),
            pltpu.VMEM((1, LANES), I32),
            pltpu.SMEM((SLOTS,), I32),
            pltpu.SMEM((1,), I32),
            pltpu.SemaphoreType.DMA((3,)),
            pltpu.SemaphoreType.DMA((5,)),
            pltpu.SemaphoreType.DMA((7,)),
            pltpu.SemaphoreType.DMA((3,)),
        ],
        compiler_params=pltpu.CompilerParams(
            collective_id=0, has_side_effects=True, vmem_limit_bytes=24 * 1024 * 1024
        ),
        name="tissue_tiles",
    )(*(in_hbm(array) for array in (slide_pixels, tissue_mask, conv_weight, conv_bias)))


def solution(mesh):
    finer = Mesh(
        mesh.devices.reshape(mesh.shape["slides"], 4, 16, 2), ("slides", "row_0", "row_1", "row_2")
    )
    return jax.shard_map(
        on_device,
        mesh=finer,
        in_specs=(P(SLIDES_ROW, None), P(SLIDES_ROW, None), P(), P()),
        out_specs=P(SLIDES_ROW, None, None),
        check_vma=False,
    )
```

```python
import functools

import jax
import jax.numpy as jnp
from jax import lax
from jax.experimental import pallas as pl
from jax.experimental.pallas import tpu as pltpu
from jax.sharding import Mesh
from jax.sharding import PartitionSpec as P

SLOTS = 8
SHIFT_MOST = 2
ROW = ("row_0", "row_1", "row_2")
SLIDES_ROW = ("slides", "row_0", "row_1", "row_2")
MESH = pl.DeviceIdType.MESH
LANES = 128
F32 = jnp.float32
BF16 = jnp.bfloat16
I32 = jnp.int32


def kernel(
    pixels,
    mask_in,
    weight_in,
    bias_in,
    out,
    top_band,
    low_band,
    mask,
    weight,
    bias,
    big,
    fat,
    lhs,
    done,
    edge_first,
    edge_last,
    first_row,
    last_row,
    first_send,
    last_send,
    above_in,
    below_in,
    above,
    below,
    tile_send,
    tile_in,
    rim_work,
    rim_send,
    rim_in,
    note_send,
    note_in,
    counts,
    line_send,
    line_in,
    order,
    excess,
    local_sem,
    send_sem,
    recv_sem,
    many_sem,
):
    x, z, c = (lax.axis_index(axis) for axis in ROW)
    planes, ring, cores = (lax.axis_size(axis) for axis in ROW)
    rows_dev, cols = mask_in.shape
    side = pixels.shape[0] // rows_dev
    tiles = rows_dev * cols
    chunks = pixels.shape[1] // (cols * LANES)
    groups = chunks // 2
    total = cols * chunks
    rank = (x * ring + z) * cores + c
    local = (x % 2) * (ring * cores) + z * cores + c
    group_size = planes * ring * cores
    follows, leads = rank > 0, rank < group_size - 1
    early = (z < 2) & follows
    hub = (z == 1) & (c == 1)
    inner = x > 0
    listens = (c == 1) & (z == 1 - inner.astype(I32))
    pair = x + 1 - 2 * (x % 2)

    def place(r):
        r = (r + group_size) % group_size
        return {"row_0": r // (ring * cores), "row_1": (r // cores) % ring, "row_2": r % cores}

    nxt, prv = place(rank + 1), place(rank - 1)

    def tell(where):
        pl.semaphore_signal(barrier, inc=1, device_id=where, device_id_type=MESH)

    barrier = pltpu.get_barrier_semaphore()
    bands = (top_band, low_band)
    copies = [
        pltpu.make_async_copy(mask_in, mask, local_sem.at[0]),
        pltpu.make_async_copy(pixels.at[side : 2 * side - 16], low_band.at[0 : side - 16], local_sem.at[2]),
        pltpu.make_async_copy(pixels.at[0:side], top_band, local_sem.at[0]),
        pltpu.make_async_copy(weight_in, weight, local_sem.at[1]),
        pltpu.make_async_copy(bias_in, bias, local_sem.at[2]),
        pltpu.make_async_copy(pixels.at[2 * side - 16 : 2 * side], low_band.at[side - 16 : side], local_sem.at[1]),
    ]
    for copy in (copies[0], copies[5], copies[1]):
        copy.start()

    @pl.when(leads)
    def _():
        tell(nxt)

    @pl.when(follows)
    def _():
        tell(prv)

    @pl.when(listens)
    def _():
        def spread(k, _):
            for core in range(cores):
                there = (k == z) & (core == c)

                @pl.when(jnp.logical_not(there))
                def _():
                    tell({"row_0": x, "row_1": k, "row_2": core})

                tell({"row_0": pair, "row_1": k, "row_2": core})
            return 0

        lax.fori_loop(0, ring, spread, 0)

    copies[0].wait()
    held = [mask[t // cols, t % cols] for t in range(tiles)]
    def keep(row, col):
        inside = (col >= 0) & (col < cols)
        return jnp.where(inside, mask[row, jnp.clip(col, 0, cols - 1)], 0).astype(F32)

    lane = lax.broadcasted_iota(I32, (1, LANES), 1)
    lower = lane < LANES // 2

    def lanes_of(col, k):
        at = jnp.clip(col * chunks + k, 0, total - 1)
        return pl.ds(at * LANES, LANES)

    def outer_row(ref, send, row, block, pick):
        for col in range(cols):
            centre = held[row * cols + col].astype(F32)
            for k in range(chunks):
                at = col * chunks + k
                line = bands[row][block : block + 16, at * LANES : (at + 1) * LANES].astype(F32)
                ref[8 + at : 9 + at, :] = line[pick : pick + 1, :] * centre
        send[...] = ref[8 : 8 + total, :].astype(BF16)

    def stage(a):
        row, col = sent_tiles[a] // cols, sent_tiles[a] % cols
        row = row if a == 0 else rows_dev - 1

        def pixels_of(k):
            low = low_band[:, lanes_of(col, k)]
            return low if a else jnp.where(row == 0, top_band[:, lanes_of(col, k)], low)

        for k in range(chunks):
            tile_send[a, k + 1] = pixels_of(k)
        right = pixels_of(chunks).astype(F32) * keep(row, col + 1)
        left = pixels_of(-1).astype(F32) * keep(row, col - 1)
        tile_send[a, 0] = jnp.where(lower, right, left).astype(BF16)

    def one(source, pick):
        return source.astype(F32)[pick : pick + 1, :]

    def inner_rim(row, pick, block, col):
        centre = keep(row, col)
        for k in range(chunks):
            yield one(bands[row][block : block + 16, lanes_of(col, k)], pick) * centre
        right = one(bands[row][block : block + 16, lanes_of(col, chunks)], pick) * keep(row, col + 1)
        left = one(bands[row][block : block + 16, lanes_of(col, -1)], pick) * keep(row, col - 1)
        yield jnp.where(lower, right, left)

    def edge_rim(ref, col):
        step = col * (chunks // 8) + 1
        body = ref[pl.ds(step * 8, chunks), :]
        for k in range(chunks):
            yield body[k : k + 1, :]
        left = ref[pl.ds((step - 1) * 8, 8), :][7:8, :]
        right = ref[pl.ds((step + chunks // 8) * 8, 8), :][0:1, :]
        yield jnp.where(lower, right, left)

    def build_big():
        copies[3].wait()
        copies[4].wait()
        nothing = jnp.zeros((64, 64), BF16)
        for dy in range(3):
            taps = [weight[dy, dx] for dx in range(3)]
            for p in (0, 1, 2, 3, 4, -1):
                parts = [taps[p - q + 1] if 0 <= p - q + 1 < 3 else nothing for q in range(4)]
                at = dy * 384 + (p if p >= 0 else 5) * 64
                big[at : at + 64, :] = jnp.concatenate(parts, axis=1)

    def bias_row():
        short = bias[...].astype(F32).reshape(1, 64)
        return jnp.concatenate([short] * 4, axis=1)

    def multiply(first=0, last=groups):
        for dy in range(3):
            rows = slice(7 + dy, 7 + dy + side)
            for g in range(first, last):
                at = slice((g - first) * side, (g - first + 1) * side)
                right = fat[2 * g + 2 if g < groups - 1 else chunks, rows, :]
                left = fat[2 * g - 1 if g > 0 else chunks, rows, :]
                lhs[at, dy * 384 : dy * 384 + 128] = fat[2 * g, rows, :].astype(BF16)
                lhs[at, dy * 384 + 128 : dy * 384 + 256] = fat[2 * g + 1, rows, :].astype(BF16)
                lhs[at, dy * 384 + 256 : dy * 384 + 384] = jnp.where(lower, right, left).astype(BF16)
        used = lhs[0 : (last - first) * side]
        return jnp.dot(used, big[...], preferred_element_type=F32) + bias_row()

    def finish(result, slot, first=0, last=groups):
        for g in range(first, last):
            part = result[(g - first) * side : (g - first + 1) * side]
            done[slot, :, g * 256 : (g + 1) * 256] = part.astype(BF16)

    def own_tiles():
        build_big()
        for row in range(rows_dev):

            def tile(col, _, row=row):
                band = bands[row]
                for k in range(chunks):
                    fat[k, 8 : 8 + side, :] = band[:, lanes_of(col, k)].astype(F32)
                right = band[:, lanes_of(col, chunks)].astype(F32) * keep(row, col + 1)
                left = band[:, lanes_of(col, -1)].astype(F32) * keep(row, col - 1)
                fat[chunks, 8 : 8 + side, :] = jnp.where(lower, right, left)
                if row == 0:
                    rim = inner_rim(1, 0, 0, col)
                    for k, line in enumerate(rim):
                        fat[k, 7:8, :] = jnp.zeros((1, LANES), F32)
                        fat[k, 8 + side : 9 + side, :] = line
                else:
                    rim = inner_rim(0, 15, side - 16, col)
                    for k, line in enumerate(rim):
                        fat[k, 7:8, :] = line
                        fat[k, 8 + side : 9 + side, :] = jnp.zeros((1, LANES), F32)
                result = multiply()
                finish(result, row * cols + col)
                for g in range(groups):
                    if row == 0:
                        edge_first[col, g : g + 1, :] = result[g * side : g * side + 1]
                    else:
                        edge_last[col, g : g + 1, :] = result[(g + 1) * side - 1 : (g + 1) * side]
                return 0

            lax.fori_loop(0, cols, tile, 0)

    def remote(source, target, sent, came, where):
        return pltpu.make_async_remote_copy(
            source, target, send_sem.at[sent], recv_sem.at[came], device_id=where, device_id_type=MESH
        )

    mine = counts.at[pl.ds(local, 1)]

    def count_to(plane):
        level = 1 - (plane > 0).astype(I32)
        return pltpu.make_async_remote_copy(
            mine, mine, many_sem.at[0], many_sem.at[1],
            device_id={"row_0": plane, "row_1": level, "row_2": 1}, device_id_type=MESH,
        )

    hearers = [(x, jnp.logical_not(listens)), (pair, listens | jnp.logical_not(listens))]

    def arrive():
        others = 2 - listens.astype(I32)
        pl.semaphore_wait(barrier, others + follows.astype(I32) + leads.astype(I32))

    def send_counts():
        for spot, used in hearers:

            @pl.when(used)
            def _(spot=spot):
                count_to(spot).start()

    note = remote(note_send, note_in, 0, 0, nxt)
    down = remote(last_send, above_in, 1, 1, nxt)
    up = remote(first_send, below_in, 2, 2, prv)
    cut = chunks // 2 + 2
    pieces = ((slice(0, cut), slice(cut, chunks + 1)), (slice(0, chunks + 1),))
    bodies = [
        [remote(tile_send.at[a, piece], tile_in.at[a, piece], 3, 4 + i - a, nxt) for i, piece in enumerate(pieces[a])]
        for a in range(SHIFT_MOST)
    ]
    rims = remote(rim_send, rim_in, 4, 6, nxt)

    def send_halo():
        @pl.when(leads)
        def _():
            down.start()

    def low_tile():
        copies[1].wait()
        for copy in copies[2:5]:
            copy.start()
        stage(1)

    def send_low():
        @pl.when(leads)
        def _():
            note.start()
            bodies[1][0].start()

    def send_top():
        stage(0)
        inner_rims()

        @pl.when(jnp.logical_not(early))
        def _():
            send_last_rim()

        @pl.when(leads)
        def _():
            bodies[0][0].start()
            bodies[0][1].start()

        outer_row(first_row, first_send, 0, 0, 0)

        @pl.when(follows)
        def _():
            up.start()

    def rim_row(rim, k):
        return rim * chunks + k if k < chunks else 3 * chunks + rim

    def set_rim(rim, k, line):
        at = rim_row(rim, k)
        rim_work[at : at + 1, :] = line

    def inner_rims():
        for k, line in enumerate(inner_rim(1, 0, 0, sent_tiles[0] % cols)):
            set_rim(0, k, line)
        for k, line in enumerate(inner_rim(0, 15, side - 16, sent_tiles[1] % cols)):
            set_rim(1, k, line)

    def send_last_rim():
        @pl.when(follows)
        def _():
            down.wait_recv()
            above[8 : 8 + total, :] = above_in[...].astype(F32)

        @pl.when(jnp.logical_not(follows))
        def _():
            above[8 : 8 + total, :] = jnp.zeros((total, LANES), F32)

        row, col = sent_tiles[0] // cols, sent_tiles[0] % cols
        for k, (outer, inner) in enumerate(zip(edge_rim(above, col), inner_rim(0, 15, side - 16, col))):
            set_rim(2, k, jnp.where(row == 0, outer, inner))
        rim_send[...] = rim_work[...].astype(BF16)

        @pl.when(leads)
        def _():
            rims.start()

    copies[5].wait()
    outer_row(last_row, last_send, rows_dev - 1, side - 16, 15)

    @pl.when(jnp.logical_not(early))
    def _():
        arrive()
        send_halo()

    upto = []
    running = jnp.int32(0)
    for t in range(tiles):
        running = running + held[t]
        upto.append(running)
    own_count = running

    def nth(k):
        return sum(((upto[t] <= k).astype(I32) for t in range(tiles - 1)), jnp.int32(0))

    counts[pl.ds(local, 1), :] = jnp.broadcast_to(own_count, (1, LANES))
    sent_tiles = [nth(own_count - SHIFT_MOST + a) for a in range(SHIFT_MOST)]
    for a in range(SHIFT_MOST):
        note_send[a : a + 1, :] = jnp.broadcast_to(sent_tiles[a], (1, LANES))
    note_send[SHIFT_MOST : SHIFT_MOST + 1, :] = jnp.broadcast_to(own_count, (1, LANES))
    zeros8 = jnp.zeros((8, LANES), F32)
    for ref in (first_row, above, below):
        ref[0:8, :] = zeros8
        ref[8 + total : 16 + total, :] = zeros8

    @pl.when(early)
    def _():
        low_tile()
        copies[2].wait()
        own_tiles()
        arrive()
        send_counts()
        send_halo()
        send_low()
        send_top()

    @pl.when(jnp.logical_not(early))
    def _():
        send_counts()
        low_tile()
        send_low()
        copies[2].wait()
        send_top()
        own_tiles()

    for k in range(SLOTS):
        order[k] = nth(jnp.int32(k))

    @pl.when(leads)
    def _():
        up.wait_recv()
        below[8 : 8 + total, :] = below_in[...].astype(F32)

    @pl.when(jnp.logical_not(leads))
    def _():
        below[8 : 8 + total, :] = jnp.zeros((total, LANES), F32)

    def join(ref, edge, dy, row, block, pick):
        half = total // 2
        even = ref[pl.ds(8, half, 2), :]
        odd = ref[pl.ds(9, half, 2), :]
        right = ref[pl.ds(10, half, 2), :]
        left = ref[pl.ds(7, half, 2), :]
        side_by = jnp.concatenate([even, odd, jnp.where(lower, right, left)], axis=1).astype(BF16)
        more = jnp.dot(side_by, big[dy * 384 : (dy + 1) * 384, :], preferred_element_type=F32)
        at_row = lax.broadcasted_iota(I32, (16, 256), 0) == pick
        for col in range(cols):
            whole = more[col * groups : (col + 1) * groups] + edge[col]
            for g in range(groups):
                span = slice(g * 256, (g + 1) * 256)
                old = done[row * cols + col, block : block + 16, span].astype(F32)
                new = jnp.where(at_row, whole[g : g + 1, :], old)
                done[row * cols + col, block : block + 16, span] = new.astype(BF16)

    join(below, edge_last, 2, rows_dev - 1, side - 16, 15)

    @pl.when(early)
    def _():
        send_last_rim()

    join(above, edge_first, 0, 0, 0, 0)

    def taken(a):
        came = jnp.max(note_in[a : a + 1, :])
        row, col = came // cols, came % cols
        came_rims = rim_in[...].astype(F32)

        def rim(which, k):
            at = rim_row(which, k)
            return came_rims[at : at + 1, :]

        for k, line in enumerate(edge_rim(first_row, col)):
            fat[k, 7:8, :] = rim(1 if a else 2, k)
            if a == 0:
                line = jnp.where(row == rows_dev - 1, line, rim(0, k))
            fat[k, 8 + side : 9 + side, :] = line
        for i, piece in enumerate(pieces[a]):
            bodies[a][i].wait_recv()
            for k in range(piece.start, piece.stop):
                fat[k - 1 if k else chunks, 8 : 8 + side, :] = tile_in[a, k].astype(F32)
            parts = len(pieces[a])
            span = (i * groups // parts, (i + 1) * groups // parts)
            result = multiply(*span)
            if a:
                finish(result, tiles, *span)
            else:
                lead_slot(result, *span)

    def lead_slot(result, first, last):
        for g in range(first, last):
            part = result[(g - first) * side : (g - first + 1) * side].astype(BF16)
            lanes = slice(g * 256, (g + 1) * 256)
            out[0, :, lanes] = jnp.where(excess[0] == SHIFT_MOST, part, out[0, :, lanes])

    @pl.when(leads)
    def _():
        for copy in (note, down, rims):
            copy.wait_send()
        pltpu.make_async_copy(tile_send, tile_send, send_sem.at[3]).wait()

    @pl.when(follows)
    def _():
        up.wait_send()

    for spot, used in hearers:

        @pl.when(used)
        def _(spot=spot):
            count_to(spot).wait_send()

    def settle(line):
        first_half = x < planes // 2
        side_wanted = (lane < local) == first_half
        part = jnp.sum(jnp.where(side_wanted & (lane < 2 * ring * cores), line, 0))
        before = jnp.where(first_half, part, SLOTS * 2 * ring * cores - part)
        excess[0] = jnp.clip(before - SLOTS * local, 0, SHIFT_MOST)

    @pl.when(follows)
    def _():
        note.wait_recv()

    @pl.when(listens)
    def _():
        others = counts.at[pl.ds(0, 2 * ring * cores - 1)]
        pltpu.make_async_copy(others, others, many_sem.at[1]).wait()
        table = counts[...]
        spot = lax.broadcasted_iota(I32, table.shape, 0) == lax.broadcasted_iota(I32, table.shape, 1)
        line = jnp.sum(jnp.where(spot, table, 0), axis=0, keepdims=True)
        line_send[...] = line
        settle(line)

    def line_to(source, level, core):
        return pltpu.make_async_remote_copy(
            source, line_in, many_sem.at[0], many_sem.at[2],
            device_id={"row_0": x, "row_1": level, "row_2": core}, device_id_type=MESH,
        )

    @pl.when(listens & inner)
    def _():
        line_to(line_send, 0, 0).start()
        line_to(line_send, 1, 1).start()

    @pl.when(hub & jnp.logical_not(inner))
    def _():
        line_in[...] = line_send[...]

    def hear():
        pltpu.make_async_copy(line_in, line_in, many_sem.at[2]).wait()
        settle(line_in[...])

    @pl.when(follows)
    def _():
        rims.wait_recv()
        taken(1)

    @pl.when((inner | (z > 0)) & jnp.logical_not(listens))
    def _():
        hear()

    @pl.when(hub)
    def _():
        def spread(k, _):
            for core in range(2):
                line_to(line_in, k, core).start()
            return 0

        line_to(line_in, 1, 0).start()
        lax.fori_loop(2, ring, spread, 0)

    @pl.when(rank == 0)
    def _():
        excess[0] = jnp.int32(0)

    @pl.when(rank == 1)
    def _():
        beside = jnp.max(note_in[SHIFT_MOST : SHIFT_MOST + 1, :])
        excess[0] = jnp.clip(beside - SLOTS, 0, SHIFT_MOST)

    shift = excess[0]

    for j in range(SLOTS):
        own = order[jnp.clip(j - shift, 0, SLOTS - 1)]
        out[j] = done[jnp.where(j == shift - 1, tiles, own)]

    @pl.when(follows)
    def _():
        taken(0)

    @pl.when(listens & inner)
    def _():
        both = counts.at[pl.ds(0, 2)]
        pltpu.make_async_copy(both, both, many_sem.at[0]).wait()

    @pl.when(hub)
    def _():
        sent = counts.at[pl.ds(0, (ring - 1) * cores - 1)]
        pltpu.make_async_copy(sent, sent, many_sem.at[0]).wait()


def in_hbm(array):
    return pltpu.with_memory_space_constraint(array, pltpu.HBM)


def on_device(slide_pixels, tissue_mask, conv_weight, conv_bias):
    rows_dev, cols = tissue_mask.shape
    side = slide_pixels.shape[0] // rows_dev
    width = slide_pixels.shape[1] // cols
    chunks = width // LANES
    groups = chunks // 2
    total = cols * chunks
    tiles = rows_dev * cols
    pair_size = 2 * lax.axis_size("row_1") * lax.axis_size("row_2")
    half = pltpu.VMEM((side, slide_pixels.shape[1]), BF16)
    strip = pltpu.VMEM((total + 16, LANES), F32)
    packed = pltpu.VMEM((total, LANES), BF16)
    rim = pltpu.VMEM((4 * chunks, LANES), BF16)
    tile_pair = pltpu.VMEM((SHIFT_MOST, chunks + 1, side, LANES), BF16)
    edge = pltpu.VMEM((cols, groups, 256), F32)
    return pl.pallas_call(
        kernel,
        out_shape=pltpu.VMEM((SLOTS, side, width), BF16),
        in_specs=[pl.BlockSpec(memory_space=pltpu.HBM)] * 4,
        out_specs=pl.BlockSpec(memory_space=pltpu.VMEM),
        scratch_shapes=[
            half,
            half,
            pltpu.SMEM((rows_dev, cols), I32),
            pltpu.VMEM(conv_weight.shape, BF16),
            pltpu.VMEM(conv_bias.shape, BF16),
            pltpu.VMEM((3 * 384, 256), BF16),
            pltpu.VMEM((chunks + 1, 48, LANES), F32),
            pltpu.VMEM((groups * side, 3 * 384), BF16),
            pltpu.VMEM((tiles + 1, side, width), BF16),
            edge,
            edge,
            strip,
            strip,
            packed,
            packed,
            packed,
            packed,
            strip,
            strip,
            tile_pair,
            tile_pair,
            pltpu.VMEM((4 * chunks, LANES), F32),
            rim,
            rim,
            pltpu.VMEM((SHIFT_MOST + 1, LANES), I32),
            pltpu.VMEM((SHIFT_MOST + 1, LANES), I32),
            pltpu.VMEM((pair_size, LANES), I32),
            pltpu.VMEM((1, LANES), I32),
            pltpu.VMEM((1, LANES), I32),
            pltpu.SMEM((SLOTS,), I32),
            pltpu.SMEM((1,), I32),
            pltpu.SemaphoreType.DMA((3,)),
            pltpu.SemaphoreType.DMA((5,)),
            pltpu.SemaphoreType.DMA((7,)),
            pltpu.SemaphoreType.DMA((3,)),
        ],
        compiler_params=pltpu.CompilerParams(
            collective_id=0, has_side_effects=True, vmem_limit_bytes=24 * 1024 * 1024
        ),
        name="tissue_tiles",
    )(*(in_hbm(array) for array in (slide_pixels, tissue_mask, conv_weight, conv_bias)))


def solution(mesh):
    finer = Mesh(
        mesh.devices.reshape(mesh.shape["slides"], 4, 16, 2), ("slides", "row_0", "row_1", "row_2")
    )
    return jax.shard_map(
        on_device,
        mesh=finer,
        in_specs=(P(SLIDES_ROW, None), P(SLIDES_ROW, None), P(), P()),
        out_specs=P(SLIDES_ROW, None, None),
        check_vma=False,
    )
```

```python
import functools

import jax
import jax.numpy as jnp
from jax import lax
from jax.experimental import pallas as pl
from jax.experimental.pallas import tpu as pltpu
from jax.sharding import Mesh
from jax.sharding import PartitionSpec as P

SLOTS = 8
SHIFT_MOST = 2
ROW = ("row_0", "row_1", "row_2")
SLIDES_ROW = ("slides", "row_0", "row_1", "row_2")
MESH = pl.DeviceIdType.MESH
LANES = 128
F32 = jnp.float32
BF16 = jnp.bfloat16
I32 = jnp.int32


def kernel(
    pixels,
    mask_in,
    weight_in,
    bias_in,
    out,
    top_band,
    low_band,
    mask,
    weight,
    bias,
    big,
    fat,
    lhs,
    done,
    edge_first,
    edge_last,
    first_row,
    last_row,
    first_send,
    last_send,
    above_in,
    below_in,
    above,
    below,
    tile_send,
    tile_in,
    rim_work,
    rim_send,
    rim_in,
    note_send,
    note_in,
    counts,
    line_send,
    line_in,
    order,
    excess,
    local_sem,
    send_sem,
    recv_sem,
    many_sem,
):
    x, z, c = (lax.axis_index(axis) for axis in ROW)
    planes, ring, cores = (lax.axis_size(axis) for axis in ROW)
    rows_dev, cols = mask_in.shape
    side = pixels.shape[0] // rows_dev
    tiles = rows_dev * cols
    chunks = pixels.shape[1] // (cols * LANES)
    groups = chunks // 2
    total = cols * chunks
    rank = (x * ring + z) * cores + c
    local = (x % 2) * (ring * cores) + z * cores + c
    group_size = planes * ring * cores
    follows, leads = rank > 0, rank < group_size - 1
    early = (z < 2) & follows
    hub = (z == 1) & (c == 1)
    inner = x > 0
    listens = (c == 1) & (z == 1 - inner.astype(I32))
    pair = x + 1 - 2 * (x % 2)

    def place(r):
        r = (r + group_size) % group_size
        return {"row_0": r // (ring * cores), "row_1": (r // cores) % ring, "row_2": r % cores}

    nxt, prv = place(rank + 1), place(rank - 1)

    def tell(where):
        pl.semaphore_signal(barrier, inc=1, device_id=where, device_id_type=MESH)

    barrier = pltpu.get_barrier_semaphore()
    bands = (top_band, low_band)
    copies = [
        pltpu.make_async_copy(mask_in, mask, local_sem.at[0]),
        pltpu.make_async_copy(pixels.at[side : 2 * side - 16], low_band.at[0 : side - 16], local_sem.at[2]),
        pltpu.make_async_copy(pixels.at[0:side], top_band, local_sem.at[0]),
        pltpu.make_async_copy(weight_in, weight, local_sem.at[1]),
        pltpu.make_async_copy(bias_in, bias, local_sem.at[2]),
        pltpu.make_async_copy(pixels.at[2 * side - 16 : 2 * side], low_band.at[side - 16 : side], local_sem.at[1]),
    ]
    for copy in (copies[0], copies[5], copies[1]):
        copy.start()

    @pl.when(leads)
    def _():
        tell(nxt)

    @pl.when(follows)
    def _():
        tell(prv)

    @pl.when(listens)
    def _():
        def spread(k, _):
            for core in range(cores):
                there = (k == z) & (core == c)

                @pl.when(jnp.logical_not(there))
                def _():
                    tell({"row_0": x, "row_1": k, "row_2": core})

                tell({"row_0": pair, "row_1": k, "row_2": core})
            return 0

        lax.fori_loop(0, ring, spread, 0)

    copies[0].wait()
    held = [mask[t // cols, t % cols] for t in range(tiles)]
    def keep(row, col):
        inside = (col >= 0) & (col < cols)
        return jnp.where(inside, mask[row, jnp.clip(col, 0, cols - 1)], 0).astype(F32)

    lane = lax.broadcasted_iota(I32, (1, LANES), 1)
    lower = lane < LANES // 2

    def lanes_of(col, k):
        at = jnp.clip(col * chunks + k, 0, total - 1)
        return pl.ds(at * LANES, LANES)

    def outer_row(ref, send, row, block, pick):
        for col in range(cols):
            centre = held[row * cols + col].astype(F32)
            for k in range(chunks):
                at = col * chunks + k
                line = bands[row][block : block + 16, at * LANES : (at + 1) * LANES].astype(F32)
                ref[8 + at : 9 + at, :] = line[pick : pick + 1, :] * centre
        send[...] = ref[8 : 8 + total, :].astype(BF16)

    def stage(a):
        row, col = sent_tiles[a] // cols, sent_tiles[a] % cols
        row = row if a == 0 else rows_dev - 1

        def pixels_of(k):
            low = low_band[:, lanes_of(col, k)]
            return low if a else jnp.where(row == 0, top_band[:, lanes_of(col, k)], low)

        for k in range(chunks):
            tile_send[a, k + 1] = pixels_of(k)
        right = pixels_of(chunks).astype(F32) * keep(row, col + 1)
        left = pixels_of(-1).astype(F32) * keep(row, col - 1)
        tile_send[a, 0] = jnp.where(lower, right, left).astype(BF16)

    def one(source, pick):
        return source.astype(F32)[pick : pick + 1, :]

    def inner_rim(row, pick, block, col):
        centre = keep(row, col)
        for k in range(chunks):
            yield one(bands[row][block : block + 16, lanes_of(col, k)], pick) * centre
        right = one(bands[row][block : block + 16, lanes_of(col, chunks)], pick) * keep(row, col + 1)
        left = one(bands[row][block : block + 16, lanes_of(col, -1)], pick) * keep(row, col - 1)
        yield jnp.where(lower, right, left)

    def edge_rim(ref, col):
        step = col * (chunks // 8) + 1
        body = ref[pl.ds(step * 8, chunks), :]
        for k in range(chunks):
            yield body[k : k + 1, :]
        left = ref[pl.ds((step - 1) * 8, 8), :][7:8, :]
        right = ref[pl.ds((step + chunks // 8) * 8, 8), :][0:1, :]
        yield jnp.where(lower, right, left)

    def build_big():
        copies[3].wait()
        copies[4].wait()
        nothing = jnp.zeros((64, 64), BF16)
        for dy in range(3):
            taps = [weight[dy, dx] for dx in range(3)]
            for p in (0, 1, 2, 3, 4, -1):
                parts = [taps[p - q + 1] if 0 <= p - q + 1 < 3 else nothing for q in range(4)]
                at = dy * 384 + (p if p >= 0 else 5) * 64
                big[at : at + 64, :] = jnp.concatenate(parts, axis=1)

    def bias_row():
        short = bias[...].astype(F32).reshape(1, 64)
        return jnp.concatenate([short] * 4, axis=1)

    def multiply(first=0, last=groups):
        for dy in range(3):
            rows = slice(7 + dy, 7 + dy + side)
            for g in range(first, last):
                at = slice((g - first) * side, (g - first + 1) * side)
                right = fat[2 * g + 2 if g < groups - 1 else chunks, rows, :]
                left = fat[2 * g - 1 if g > 0 else chunks, rows, :]
                lhs[at, dy * 384 : dy * 384 + 128] = fat[2 * g, rows, :].astype(BF16)
                lhs[at, dy * 384 + 128 : dy * 384 + 256] = fat[2 * g + 1, rows, :].astype(BF16)
                lhs[at, dy * 384 + 256 : dy * 384 + 384] = jnp.where(lower, right, left).astype(BF16)
        used = lhs[0 : (last - first) * side]
        return jnp.dot(used, big[...], preferred_element_type=F32) + bias_row()

    def finish(result, slot, first=0, last=groups):
        for g in range(first, last):
            part = result[(g - first) * side : (g - first + 1) * side]
            done[slot, :, g * 256 : (g + 1) * 256] = part.astype(BF16)

    def own_tiles():
        build_big()
        for row in range(rows_dev):

            def tile(col, _, row=row):
                band = bands[row]
                for k in range(chunks):
                    fat[k, 8 : 8 + side, :] = band[:, lanes_of(col, k)].astype(F32)
                right = band[:, lanes_of(col, chunks)].astype(F32) * keep(row, col + 1)
                left = band[:, lanes_of(col, -1)].astype(F32) * keep(row, col - 1)
                fat[chunks, 8 : 8 + side, :] = jnp.where(lower, right, left)
                if row == 0:
                    rim = inner_rim(1, 0, 0, col)
                    for k, line in enumerate(rim):
                        fat[k, 7:8, :] = jnp.zeros((1, LANES), F32)
                        fat[k, 8 + side : 9 + side, :] = line
                else:
                    rim = inner_rim(0, 15, side - 16, col)
                    for k, line in enumerate(rim):
                        fat[k, 7:8, :] = line
                        fat[k, 8 + side : 9 + side, :] = jnp.zeros((1, LANES), F32)
                result = multiply()
                finish(result, row * cols + col)
                for g in range(groups):
                    if row == 0:
                        edge_first[col, g : g + 1, :] = result[g * side : g * side + 1]
                    else:
                        edge_last[col, g : g + 1, :] = result[(g + 1) * side - 1 : (g + 1) * side]
                return 0

            lax.fori_loop(0, cols, tile, 0)

    def remote(source, target, sent, came, where):
        return pltpu.make_async_remote_copy(
            source, target, send_sem.at[sent], recv_sem.at[came], device_id=where, device_id_type=MESH
        )

    mine = counts.at[pl.ds(local, 1)]

    def count_to(plane):
        level = 1 - (plane > 0).astype(I32)
        return pltpu.make_async_remote_copy(
            mine, mine, many_sem.at[0], many_sem.at[1],
            device_id={"row_0": plane, "row_1": level, "row_2": 1}, device_id_type=MESH,
        )

    hearers = [(x, jnp.logical_not(listens)), (pair, listens | jnp.logical_not(listens))]

    def arrive():
        others = 2 - listens.astype(I32)
        pl.semaphore_wait(barrier, others + follows.astype(I32) + leads.astype(I32))

    def send_counts():
        for spot, used in hearers:

            @pl.when(used)
            def _(spot=spot):
                count_to(spot).start()

    note = remote(note_send, note_in, 0, 0, nxt)
    down = remote(last_send, above_in, 1, 1, nxt)
    up = remote(first_send, below_in, 2, 2, prv)
    cut = chunks // 2 + 2
    pieces = ((slice(0, cut), slice(cut, chunks + 1)), (slice(0, chunks + 1),))
    bodies = [
        [remote(tile_send.at[a, piece], tile_in.at[a, piece], 3, 4 + i - a, nxt) for i, piece in enumerate(pieces[a])]
        for a in range(SHIFT_MOST)
    ]
    rims = remote(rim_send, rim_in, 4, 6, nxt)

    def send_halo():
        @pl.when(leads)
        def _():
            down.start()

    def low_tile():
        copies[1].wait()
        for copy in copies[2:5]:
            copy.start()
        stage(1)

    def send_low():
        @pl.when(leads)
        def _():
            note.start()
            bodies[1][0].start()

    def send_top():
        stage(0)
        inner_rims()

        @pl.when(jnp.logical_not(early))
        def _():
            send_last_rim()

        @pl.when(leads)
        def _():
            bodies[0][0].start()
            bodies[0][1].start()

        outer_row(first_row, first_send, 0, 0, 0)

        @pl.when(follows)
        def _():
            up.start()

    def rim_row(rim, k):
        return rim * chunks + k if k < chunks else 3 * chunks + rim

    def set_rim(rim, k, line):
        at = rim_row(rim, k)
        rim_work[at : at + 1, :] = line

    def inner_rims():
        for k, line in enumerate(inner_rim(1, 0, 0, sent_tiles[0] % cols)):
            set_rim(0, k, line)
        for k, line in enumerate(inner_rim(0, 15, side - 16, sent_tiles[1] % cols)):
            set_rim(1, k, line)

    def send_last_rim():
        @pl.when(follows)
        def _():
            down.wait_recv()
            above[8 : 8 + total, :] = above_in[...].astype(F32)

        @pl.when(jnp.logical_not(follows))
        def _():
            above[8 : 8 + total, :] = jnp.zeros((total, LANES), F32)

        row, col = sent_tiles[0] // cols, sent_tiles[0] % cols
        for k, (outer, inner) in enumerate(zip(edge_rim(above, col), inner_rim(0, 15, side - 16, col))):
            set_rim(2, k, jnp.where(row == 0, outer, inner))
        rim_send[...] = rim_work[...].astype(BF16)

        @pl.when(leads)
        def _():
            rims.start()

    copies[5].wait()
    outer_row(last_row, last_send, rows_dev - 1, side - 16, 15)

    @pl.when(jnp.logical_not(early))
    def _():
        arrive()
        send_halo()

    upto = []
    running = jnp.int32(0)
    for t in range(tiles):
        running = running + held[t]
        upto.append(running)
    own_count = running

    def nth(k):
        return sum(((upto[t] <= k).astype(I32) for t in range(tiles - 1)), jnp.int32(0))

    counts[pl.ds(local, 1), :] = jnp.broadcast_to(own_count, (1, LANES))
    sent_tiles = [nth(own_count - SHIFT_MOST + a) for a in range(SHIFT_MOST)]
    for a in range(SHIFT_MOST):
        note_send[a : a + 1, :] = jnp.broadcast_to(sent_tiles[a], (1, LANES))
    note_send[SHIFT_MOST : SHIFT_MOST + 1, :] = jnp.broadcast_to(own_count, (1, LANES))
    zeros8 = jnp.zeros((8, LANES), F32)
    for ref in (first_row, above, below):
        ref[0:8, :] = zeros8
        ref[8 + total : 16 + total, :] = zeros8

    @pl.when(early)
    def _():
        low_tile()
        copies[2].wait()
        own_tiles()
        arrive()
        send_counts()
        send_halo()
        send_low()
        send_top()

    @pl.when(jnp.logical_not(early))
    def _():
        send_counts()
        low_tile()
        send_low()
        copies[2].wait()
        send_top()
        own_tiles()

    for k in range(SLOTS):
        order[k] = nth(jnp.int32(k))

    @pl.when(leads)
    def _():
        up.wait_recv()
        below[8 : 8 + total, :] = below_in[...].astype(F32)

    @pl.when(jnp.logical_not(leads))
    def _():
        below[8 : 8 + total, :] = jnp.zeros((total, LANES), F32)

    def join(ref, edge, dy, row, block, pick):
        half = total // 2
        even = ref[pl.ds(8, half, 2), :]
        odd = ref[pl.ds(9, half, 2), :]
        right = ref[pl.ds(10, half, 2), :]
        left = ref[pl.ds(7, half, 2), :]
        side_by = jnp.concatenate([even, odd, jnp.where(lower, right, left)], axis=1).astype(BF16)
        more = jnp.dot(side_by, big[dy * 384 : (dy + 1) * 384, :], preferred_element_type=F32)
        at_row = lax.broadcasted_iota(I32, (16, 256), 0) == pick
        for col in range(cols):
            whole = more[col * groups : (col + 1) * groups] + edge[col]
            for g in range(groups):
                span = slice(g * 256, (g + 1) * 256)
                old = done[row * cols + col, block : block + 16, span].astype(F32)
                new = jnp.where(at_row, whole[g : g + 1, :], old)
                done[row * cols + col, block : block + 16, span] = new.astype(BF16)

    join(below, edge_last, 2, rows_dev - 1, side - 16, 15)

    @pl.when(early)
    def _():
        send_last_rim()

    join(above, edge_first, 0, 0, 0, 0)

    def taken(a):
        came = jnp.max(note_in[a : a + 1, :])
        row, col = came // cols, came % cols
        came_rims = rim_in[...].astype(F32)

        def rim(which, k):
            at = rim_row(which, k)
            return came_rims[at : at + 1, :]

        for k, line in enumerate(edge_rim(first_row, col)):
            fat[k, 7:8, :] = rim(1 if a else 2, k)
            if a == 0:
                line = jnp.where(row == rows_dev - 1, line, rim(0, k))
            fat[k, 8 + side : 9 + side, :] = line
        for i, piece in enumerate(pieces[a]):
            bodies[a][i].wait_recv()
            for k in range(piece.start, piece.stop):
                fat[k - 1 if k else chunks, 8 : 8 + side, :] = tile_in[a, k].astype(F32)
            parts = len(pieces[a])
            span = (i * groups // parts, (i + 1) * groups // parts)
            result = multiply(*span)
            if a:
                finish(result, tiles, *span)
            else:
                lead_slot(result, *span)

    def lead_slot(result, first, last):
        for g in range(first, last):
            part = result[(g - first) * side : (g - first + 1) * side].astype(BF16)
            lanes = slice(g * 256, (g + 1) * 256)
            out[0, :, lanes] = jnp.where(excess[0] == SHIFT_MOST, part, out[0, :, lanes])

    @pl.when(leads)
    def _():
        for copy in (note, down, rims):
            copy.wait_send()
        pltpu.make_async_copy(tile_send, tile_send, send_sem.at[3]).wait()

    @pl.when(follows)
    def _():
        up.wait_send()

    for spot, used in hearers:

        @pl.when(used)
        def _(spot=spot):
            count_to(spot).wait_send()

    def settle(line):
        first_half = x < planes // 2
        side_wanted = (lane < local) == first_half
        part = jnp.sum(jnp.where(side_wanted & (lane < 2 * ring * cores), line, 0))
        before = jnp.where(first_half, part, SLOTS * 2 * ring * cores - part)
        excess[0] = jnp.clip(before - SLOTS * local, 0, SHIFT_MOST)

    @pl.when(follows)
    def _():
        note.wait_recv()

    @pl.when(listens)
    def _():
        others = counts.at[pl.ds(0, 2 * ring * cores - 1)]
        pltpu.make_async_copy(others, others, many_sem.at[1]).wait()
        table = counts[...]
        spot = lax.broadcasted_iota(I32, table.shape, 0) == lax.broadcasted_iota(I32, table.shape, 1)
        line = jnp.sum(jnp.where(spot, table, 0), axis=0, keepdims=True)
        line_send[...] = line
        settle(line)

    def line_to(source, level, core):
        return pltpu.make_async_remote_copy(
            source, line_in, many_sem.at[0], many_sem.at[1],
            device_id={"row_0": x, "row_1": level, "row_2": core}, device_id_type=MESH,
        )

    @pl.when(listens & inner)
    def _():
        line_to(line_send, 0, 0).start()
        line_to(line_send, 1, 1).start()

    @pl.when(hub & jnp.logical_not(inner))
    def _():
        line_in[...] = line_send[...]

    def hear():
        pltpu.make_async_copy(line_in, line_in, many_sem.at[1]).wait()
        settle(line_in[...])

    @pl.when(follows)
    def _():
        rims.wait_recv()
        taken(1)

    @pl.when((inner | (z > 0)) & jnp.logical_not(listens))
    def _():
        hear()

    @pl.when(hub)
    def _():
        def spread(k, _):
            for core in range(2):
                line_to(line_in, k, core).start()
            return 0

        line_to(line_in, 1, 0).start()
        lax.fori_loop(2, ring, spread, 0)

    @pl.when(rank == 0)
    def _():
        excess[0] = jnp.int32(0)

    @pl.when(rank == 1)
    def _():
        beside = jnp.max(note_in[SHIFT_MOST : SHIFT_MOST + 1, :])
        excess[0] = jnp.clip(beside - SLOTS, 0, SHIFT_MOST)

    shift = excess[0]

    for j in range(SLOTS):
        own = order[jnp.clip(j - shift, 0, SLOTS - 1)]
        out[j] = done[jnp.where(j == shift - 1, tiles, own)]

    @pl.when(follows)
    def _():
        taken(0)

    @pl.when(listens & inner)
    def _():
        both = counts.at[pl.ds(0, 2)]
        pltpu.make_async_copy(both, both, many_sem.at[0]).wait()

    @pl.when(hub)
    def _():
        sent = counts.at[pl.ds(0, (ring - 1) * cores - 1)]
        pltpu.make_async_copy(sent, sent, many_sem.at[0]).wait()


def in_hbm(array):
    return pltpu.with_memory_space_constraint(array, pltpu.HBM)


def on_device(slide_pixels, tissue_mask, conv_weight, conv_bias):
    rows_dev, cols = tissue_mask.shape
    side = slide_pixels.shape[0] // rows_dev
    width = slide_pixels.shape[1] // cols
    chunks = width // LANES
    groups = chunks // 2
    total = cols * chunks
    tiles = rows_dev * cols
    pair_size = 2 * lax.axis_size("row_1") * lax.axis_size("row_2")
    half = pltpu.VMEM((side, slide_pixels.shape[1]), BF16)
    strip = pltpu.VMEM((total + 16, LANES), F32)
    packed = pltpu.VMEM((total, LANES), BF16)
    rim = pltpu.VMEM((4 * chunks, LANES), BF16)
    tile_pair = pltpu.VMEM((SHIFT_MOST, chunks + 1, side, LANES), BF16)
    edge = pltpu.VMEM((cols, groups, 256), F32)
    return pl.pallas_call(
        kernel,
        out_shape=pltpu.VMEM((SLOTS, side, width), BF16),
        in_specs=[pl.BlockSpec(memory_space=pltpu.HBM)] * 4,
        out_specs=pl.BlockSpec(memory_space=pltpu.VMEM),
        scratch_shapes=[
            half,
            half,
            pltpu.SMEM((rows_dev, cols), I32),
            pltpu.VMEM(conv_weight.shape, BF16),
            pltpu.VMEM(conv_bias.shape, BF16),
            pltpu.VMEM((3 * 384, 256), BF16),
            pltpu.VMEM((chunks + 1, 48, LANES), F32),
            pltpu.VMEM((groups * side, 3 * 384), BF16),
            pltpu.VMEM((tiles + 1, side, width), BF16),
            edge,
            edge,
            strip,
            strip,
            packed,
            packed,
            packed,
            packed,
            strip,
            strip,
            tile_pair,
            tile_pair,
            pltpu.VMEM((4 * chunks, LANES), F32),
            rim,
            rim,
            pltpu.VMEM((SHIFT_MOST + 1, LANES), I32),
            pltpu.VMEM((SHIFT_MOST + 1, LANES), I32),
            pltpu.VMEM((pair_size, LANES), I32),
            pltpu.VMEM((1, LANES), I32),
            pltpu.VMEM((1, LANES), I32),
            pltpu.SMEM((SLOTS,), I32),
            pltpu.SMEM((1,), I32),
            pltpu.SemaphoreType.DMA((3,)),
            pltpu.SemaphoreType.DMA((5,)),
            pltpu.SemaphoreType.DMA((7,)),
            pltpu.SemaphoreType.DMA((2,)),
        ],
        compiler_params=pltpu.CompilerParams(
            collective_id=0,
            has_side_effects=True,
            vmem_limit_bytes=24 * 1024 * 1024,
        ),
        name="tissue_tiles",
    )(*(in_hbm(array) for array in (slide_pixels, tissue_mask, conv_weight, conv_bias)))


def solution(mesh):
    finer = Mesh(
        mesh.devices.reshape(mesh.shape["slides"], 4, 16, 2), ("slides", "row_0", "row_1", "row_2")
    )
    return jax.shard_map(
        on_device,
        mesh=finer,
        in_specs=(P(SLIDES_ROW, None), P(SLIDES_ROW, None), P(), P()),
        out_specs=P(SLIDES_ROW, None, None),
        check_vma=False,
    )
```
